32 devices in a mesh: pod: 2 (over x), dp: 4 (over z), tp: 4 (over y, core).
Axes of the slice: x: 2, y: 2, z: 4, core: 2. Of those that a mesh axis runs over, the one named last changes fastest.
Arguments:
- x_saved: bfloat16 [12288, 1024], P(('pod', 'dp')), parts along dimension 0
- h_saved: bfloat16 [12288, 1024], P(('pod', 'dp')), parts along dimension 0
- mean_one: float32 [12288], P(('pod', 'dp')), parts along dimension 0
- rstd_one: float32 [12288], P(('pod', 'dp')), parts along dimension 0
- mean_two: float32 [12288], P(('pod', 'dp')), parts along dimension 0
- rstd_two: float32 [12288], P(('pod', 'dp')), parts along dimension 0
- gain_one: bfloat16 [1024], replicated
- gain_two: bfloat16 [1024], replicated
- grad_y: bfloat16 [12288, 1024], P(('pod', 'dp')), parts along dimension 0
- w_qkv: bfloat16 [1024, 3, 16, 64], P(None, None, 'tp')
- w_proj: bfloat16 [16, 64, 1024], P('tp')
- w_up: bfloat16 [1024, 4096], P(None, 'tp')
- w_down: bfloat16 [4096, 1024], P('tp')
Outputs:
- output 1: bfloat16 [12288, 1024], P(('pod', 'dp')), parts along dimension 0
- output 2: bfloat16 [2048, 3, 16, 64], P('pod', None, 'tp'), parts along dimension 0
- output 3: bfloat16 [32, 64, 1024], P(('pod', 'tp')), parts along dimension 0
- output 4: bfloat16 [2048, 4096], P('pod', 'tp'), parts along dimension 0
- output 5: bfloat16 [8192, 1024], P(('pod', 'tp')), parts along dimension 0
There are 2 independent parts. The reference program is written for one: setup_inputs(seed, part) draws one part's arguments, and reference() takes and returns one part's arrays. A program takes and returns all parts, laid end to end along the dimension named above; an argument that names none is the same for every part.
All inputs are finite; a program needn't handle non-finite values.
Results may differ from the reference program's by a relative error of at most 0.0170911.
Values are sent between devices in bfloat16 or wider.
A program may use at most 1 GiB of HBM per device.

```python
import math
import jax
import jax.numpy as jnp
from jax import lax

MODEL_DIM = 1024
NUM_HEADS = 16
FFN_DIM = 4096
TOKENS = 1536
DATA_WAYS = 4

HEAD_DIM = MODEL_DIM // NUM_HEADS
ROW_COUNT = DATA_WAYS * TOKENS
QK_GAIN = (2.0 * math.log(TOKENS)) ** 0.25
GELU_C = math.sqrt(2.0 / math.pi)


def saved_stats(rows_wide):
    row_mean = jnp.mean(rows_wide, axis=-1)
    row_var = jnp.mean(jnp.square(rows_wide - row_mean[:, None]), axis=-1)
    return row_mean, 1.0 / jnp.sqrt(row_var + 1e-5)


def setup_inputs(seed: int = 0, part: int = 0) -> dict:
    shared_keys = jax.random.split(jax.random.key(seed), 6)
    own_keys = jax.random.split(jax.random.fold_in(jax.random.key(seed + 1), part), 7)
    x_rows = jnp.exp(jax.random.uniform(own_keys[3], (ROW_COUNT, 1), jnp.float32, -0.7, 0.7))
    h_rows = jnp.exp(jax.random.uniform(own_keys[4], (ROW_COUNT, 1), jnp.float32, -0.7, 0.7))
    x_shift = 0.5 * jax.random.normal(own_keys[5], (ROW_COUNT, 1), jnp.float32)
    h_shift = 0.5 * jax.random.normal(own_keys[6], (ROW_COUNT, 1), jnp.float32)
    x_saved = (jax.random.normal(own_keys[0], (ROW_COUNT, MODEL_DIM), jnp.float32) * x_rows + x_shift).astype(jnp.bfloat16)
    h_saved = (jax.random.normal(own_keys[1], (ROW_COUNT, MODEL_DIM), jnp.float32) * h_rows + h_shift).astype(jnp.bfloat16)
    grad_y = jax.random.normal(own_keys[2], (ROW_COUNT, MODEL_DIM), jnp.float32).astype(jnp.bfloat16)
    mean_one, rstd_one = saved_stats(x_saved.astype(jnp.float32))
    mean_two, rstd_two = saved_stats(h_saved.astype(jnp.float32))
    gain_one = (1.0 + 0.3 * jax.random.normal(shared_keys[0], (MODEL_DIM,), jnp.float32)).astype(jnp.bfloat16)
    gain_two = (1.0 + 0.3 * jax.random.normal(shared_keys[1], (MODEL_DIM,), jnp.float32)).astype(jnp.bfloat16)
    qkv_scale = jnp.array([QK_GAIN, QK_GAIN, 1.0], jnp.float32)[None, :, None, None] * MODEL_DIM ** -0.5
    w_qkv = (jax.random.normal(shared_keys[2], (MODEL_DIM, 3, NUM_HEADS, HEAD_DIM), jnp.float32) * qkv_scale).astype(jnp.bfloat16)
    w_proj = (jax.random.normal(shared_keys[3], (NUM_HEADS, HEAD_DIM, MODEL_DIM), jnp.float32) * MODEL_DIM ** -0.5).astype(jnp.bfloat16)
    w_up = (jax.random.normal(shared_keys[4], (MODEL_DIM, FFN_DIM), jnp.float32) * MODEL_DIM ** -0.5).astype(jnp.bfloat16)
    w_down = (jax.random.normal(shared_keys[5], (FFN_DIM, MODEL_DIM), jnp.float32) * FFN_DIM ** -0.5).astype(jnp.bfloat16)
    return {'x_saved': x_saved, 'h_saved': h_saved, 'mean_one': mean_one, 'rstd_one': rstd_one,
            'mean_two': mean_two, 'rstd_two': rstd_two, 'gain_one': gain_one, 'gain_two': gain_two,
            'grad_y': grad_y, 'w_qkv': w_qkv, 'w_proj': w_proj, 'w_up': w_up, 'w_down': w_down}


def layer_norm(row_vals, row_mean, row_rstd, gain_vec):
    x_hat = (row_vals.astype(jnp.float32) - row_mean[:, None]) * row_rstd[:, None]
    return x_hat, (x_hat * gain_vec.astype(jnp.float32)).astype(jnp.bfloat16)


def norm_back(d_norm, x_hat, row_rstd, gain_vec):
    scaled = d_norm * gain_vec.astype(jnp.float32)
    scaled_mean = jnp.mean(scaled, axis=-1, keepdims=True)
    proj_mean = jnp.mean(scaled * x_hat, axis=-1, keepdims=True)
    return row_rstd[:, None] * (scaled - scaled_mean - x_hat * proj_mean)


def gelu_pair(pre_act):
    pre_wide = pre_act.astype(jnp.float32)
    tanh_val = jnp.tanh(GELU_C * (pre_wide + 0.044715 * pre_wide * pre_wide * pre_wide))
    gelu_val = 0.5 * pre_wide * (1.0 + tanh_val)
    gelu_slope = 0.5 * (1.0 + tanh_val) + 0.5 * pre_wide * (1.0 - tanh_val * tanh_val) * GELU_C * (1.0 + 0.134145 * pre_wide * pre_wide)
    return gelu_val, gelu_slope


def head_pass(head_in):
    qkv_head, dout_head = head_in
    q_head = qkv_head[:, 0]
    k_head = qkv_head[:, 1]
    v_head = qkv_head[:, 2]
    scores = jnp.dot(q_head, k_head.T, preferred_element_type=jnp.float32) * HEAD_DIM ** -0.5
    row_ids = lax.broadcasted_iota(jnp.int32, (TOKENS, TOKENS), 0)
    col_ids = lax.broadcasted_iota(jnp.int32, (TOKENS, TOKENS), 1)
    scores = jnp.where(col_ids <= row_ids, scores, -1e30)
    shifted = jnp.exp(scores - jnp.max(scores, axis=-1, keepdims=True))
    prob_mat = shifted / jnp.sum(shifted, axis=-1, keepdims=True)
    prob_lo = prob_mat.astype(jnp.bfloat16)
    head_out = jnp.dot(prob_lo, v_head, preferred_element_type=jnp.float32).astype(jnp.bfloat16)
    dv_head = jnp.dot(prob_lo.T, dout_head, preferred_element_type=jnp.float32).astype(jnp.bfloat16)
    d_probs = jnp.dot(dout_head, v_head.T, preferred_element_type=jnp.float32)
    d_scores = (prob_mat * (d_probs - jnp.sum(prob_mat * d_probs, axis=-1, keepdims=True)) * HEAD_DIM ** -0.5).astype(jnp.bfloat16)
    dq_head = jnp.dot(d_scores, k_head, preferred_element_type=jnp.float32).astype(jnp.bfloat16)
    dk_head = jnp.dot(d_scores.T, q_head, preferred_element_type=jnp.float32).astype(jnp.bfloat16)
    return head_out, jnp.stack([dq_head, dk_head, dv_head], axis=1)


def reference(x_saved, h_saved, mean_one, rstd_one, mean_two, rstd_two, gain_one, gain_two, grad_y, w_qkv, w_proj, w_up, w_down):
    qkv_wide = w_qkv.astype(jnp.float32)
    proj_wide = w_proj.astype(jnp.float32)

    def seq_pass(carry, seq_in):
        acc_qkv, acc_proj, acc_up, acc_down = carry
        x_seq, h_seq, mean_a, rstd_a, mean_b, rstd_b, dy_seq = seq_in
        hat_two, norm_two = layer_norm(h_seq, mean_b, rstd_b, gain_two)
        pre_act = jnp.dot(norm_two, w_up, preferred_element_type=jnp.float32).astype(jnp.bfloat16)
        gelu_val, gelu_slope = gelu_pair(pre_act)
        act_out = gelu_val.astype(jnp.bfloat16)
        d_pre = (jnp.dot(dy_seq, w_down.T, preferred_element_type=jnp.float32) * gelu_slope).astype(jnp.bfloat16)
        acc_up = acc_up + jnp.dot(norm_two.T, d_pre, preferred_element_type=jnp.float32)
        acc_down = acc_down + jnp.dot(act_out.T, dy_seq, preferred_element_type=jnp.float32)
        d_norm_two = jnp.dot(d_pre, w_up.T, preferred_element_type=jnp.float32)
        d_mid = dy_seq.astype(jnp.float32) + norm_back(d_norm_two, hat_two, rstd_b, gain_two)
        d_mid_lo = d_mid.astype(jnp.bfloat16)
        hat_one, norm_one = layer_norm(x_seq, mean_a, rstd_a, gain_one)
        qkv_heads = jnp.einsum('td,dche->tche', norm_one.astype(jnp.float32), qkv_wide).astype(jnp.bfloat16)
        d_attn = jnp.einsum('td,hed->the', d_mid_lo.astype(jnp.float32), proj_wide).astype(jnp.bfloat16)
        head_outs, head_grads = lax.map(head_pass, (jnp.moveaxis(qkv_heads, 2, 0), jnp.moveaxis(d_attn, 1, 0)))
        attn_out = jnp.moveaxis(head_outs, 0, 1)
        d_qkv = jnp.moveaxis(head_grads, 0, 2).astype(jnp.float32)
        acc_proj = acc_proj + jnp.einsum('the,td->hed', attn_out.astype(jnp.float32), d_mid_lo.astype(jnp.float32))
        acc_qkv = acc_qkv + jnp.einsum('td,tche->dche', norm_one.astype(jnp.float32), d_qkv)
        d_norm_one = jnp.einsum('tche,dche->td', d_qkv, qkv_wide)
        grad_x = (d_mid + norm_back(d_norm_one, hat_one, rstd_a, gain_one)).astype(jnp.bfloat16)
        return (acc_qkv, acc_proj, acc_up, acc_down), grad_x

    zero_sums = (jnp.zeros((MODEL_DIM, 3, NUM_HEADS, HEAD_DIM), jnp.float32),
                 jnp.zeros((NUM_HEADS, HEAD_DIM, MODEL_DIM), jnp.float32),
                 jnp.zeros((MODEL_DIM, FFN_DIM), jnp.float32),
                 jnp.zeros((FFN_DIM, MODEL_DIM), jnp.float32))
    seq_inputs = (x_saved.reshape(DATA_WAYS, TOKENS, MODEL_DIM), h_saved.reshape(DATA_WAYS, TOKENS, MODEL_DIM),
                  mean_one.reshape(DATA_WAYS, TOKENS), rstd_one.reshape(DATA_WAYS, TOKENS),
                  mean_two.reshape(DATA_WAYS, TOKENS), rstd_two.reshape(DATA_WAYS, TOKENS),
                  grad_y.reshape(DATA_WAYS, TOKENS, MODEL_DIM))
    grad_sums, grad_rows = lax.scan(seq_pass, zero_sums, seq_inputs)
    acc_qkv, acc_proj, acc_up, acc_down = grad_sums
    return (grad_rows.reshape(ROW_COUNT, MODEL_DIM), acc_qkv.astype(jnp.bfloat16), acc_proj.astype(jnp.bfloat16),
            acc_up.astype(jnp.bfloat16), acc_down.astype(jnp.bfloat16))
```

```python
import functools
import math
import jax
import jax.numpy as jnp
from jax import lax
from jax.experimental import pallas as pl
from jax.experimental.pallas import tpu as pltpu
from jax.sharding import PartitionSpec as P

GELU_C = math.sqrt(2.0 / math.pi)
MESH = pl.DeviceIdType.MESH
F32 = jnp.float32
BF16 = jnp.bfloat16

TOK = 1536
DIM = 1024
BLK = 256
HALF = TOK // 2
NBLK = TOK // BLK
HBLK = HALF // BLK
CROWS = 32
ROWS = 3072
CHUNKS = ROWS // (2 * CROWS)
SLOTS = 16
STAGES = 8
LAG = 2
DP = 4
STEPS = CHUNKS + 2 * LAG * (DP - 1)


def dot_nn(a, b):
    return lax.dot_general(a, b, (((1,), (0,)), ((), ())), preferred_element_type=F32)


def dot_nt(a, b):
    return lax.dot_general(a, b, (((1,), (1,)), ((), ())), preferred_element_type=F32)


def dot_tn(a, b):
    return lax.dot_general(a, b, (((0,), (0,)), ((), ())), preferred_element_type=F32)


def layer_kernel(x_ref, h_ref, dy_ref, st_ref, gn_ref, wq_ref, wo_ref, w1_ref, w2_ref,
                 dx_ref, fb_ref,
                 gb, land, stage, nrm, part, recv_a, recv_b, recv_c, dh_f, dh_b,
                 ch_send, ch_recv, ch_free, fb_send, fb_recv, st_copy,
                 pa_send, pa_recv, pb_send, pb_recv, pd_send, pd_recv, dx_copy):
    pod, z, tp = lax.axis_index('pod'), lax.axis_index('dp'), lax.axis_index('tp')
    core = lax.rem(tp, 2)
    mate = (pod, z, tp + 1 - 2 * core)
    peer = (pod, z, lax.rem(tp + 2, 4))
    z_hi = jnp.minimum(z + 1, DP - 1)
    z_lo = jnp.maximum(z - 1, 0)
    own0 = core * HALF
    par0 = HALF - own0

    barrier = pltpu.get_barrier_semaphore()
    for dev in (mate, peer):
        pl.semaphore_signal(barrier, inc=1, device_id=dev, device_id_type=MESH)
    pl.when(z < DP - 1)(lambda: pl.semaphore_signal(barrier, inc=1, device_id=(pod, z_hi, tp), device_id_type=MESH))
    pl.when(z > 0)(lambda: pl.semaphore_signal(barrier, inc=1, device_id=(pod, z_lo, tp), device_id_type=MESH))
    pl.semaphore_wait(barrier, 2 + jnp.where(z < DP - 1, 1, 0) + jnp.where(z > 0, 1, 0))

    def way_of(way):
        if way == 0:
            return z, (pod, z_hi, tp), (pod, z_lo, tp)
        return DP - 1 - z, (pod, z_lo, tp), (pod, z_hi, tp)

    def rows_of(way, c):
        return pl.ds(pl.multiple_of(c * (2 * CROWS) + way * CROWS, CROWS), CROWS)

    def chain_copy(way, c, nxt):
        slot = lax.rem(c, SLOTS)
        return pltpu.make_async_remote_copy(
            src_ref=gb.at[rows_of(way, c)], dst_ref=land.at[way, slot], send_sem=ch_send.at[way, slot],
            recv_sem=ch_recv.at[way, slot], device_id=nxt, device_id_type=MESH)

    def total_copy(way, c, prv):
        return pltpu.make_async_remote_copy(
            src_ref=stage.at[way, lax.rem(c, STAGES)], dst_ref=fb_ref.at[rows_of(way, c)], send_sem=fb_send.at[way, c],
            recv_sem=fb_recv.at[way, c], device_id=prv, device_id_type=MESH)

    def pass_copy(way, c, prv):
        return pltpu.make_async_remote_copy(
            src_ref=fb_ref.at[rows_of(way, c)], dst_ref=fb_ref.at[rows_of(way, c)], send_sem=fb_send.at[way, c],
            recv_sem=fb_recv.at[way, c], device_id=prv, device_id_type=MESH)

    def keep_copy(way, c):
        slot = lax.rem(c, STAGES)
        return pltpu.make_async_copy(stage.at[way, slot], fb_ref.at[rows_of(way, c)], st_copy.at[way, slot])

    def chain_step(s):
        for way in (0, 1):
            pos, nxt, prv = way_of(way)
            c = s - LAG * pos

            @pl.when((c >= 0) & (c < CHUNKS))
            def _():
                @pl.when(pos > 0)
                def _():
                    chain_copy(way, c, nxt).wait_recv()
                    gb[rows_of(way, c), :] += land[way, lax.rem(c, SLOTS)]

                    @pl.when(c < CHUNKS - SLOTS)
                    def _():
                        pl.semaphore_signal(ch_free.at[way], inc=1, device_id=prv, device_id_type=MESH)

                @pl.when(pos < DP - 1)
                def _():
                    @pl.when(c >= SLOTS)
                    def _():
                        pl.semaphore_wait(ch_free.at[way], 1)
                        chain_copy(way, c - SLOTS, nxt).wait_send()
                    chain_copy(way, c, nxt).start()

                @pl.when(pos == DP - 1)
                def _():
                    @pl.when(c >= STAGES)
                    def _():
                        total_copy(way, c - STAGES, prv).wait_send()
                        keep_copy(way, c - STAGES).wait()
                    stage[way, lax.rem(c, STAGES)] = gb[rows_of(way, c), :].astype(BF16)
                    total_copy(way, c, prv).start()
                    keep_copy(way, c).start()

            c2 = s - LAG * (2 * (DP - 1) - pos)

            @pl.when((pos < DP - 1) & (c2 >= 0) & (c2 < CHUNKS))
            def _():
                pass_copy(way, c2, prv).wait_recv()

                @pl.when(pos > 0)
                def _():
                    pass_copy(way, c2, prv).start()

    def chain_steps(s0, n):
        def body(k, carry):
            chain_step(s0 + k)
            return carry
        lax.fori_loop(0, n, body, 0)

    def chain_end():
        for way in (0, 1):
            pos, nxt, prv = way_of(way)

            @pl.when(pos < DP - 1)
            def _():
                def body(c, carry):
                    chain_copy(way, c, nxt).wait_send()
                    return carry
                lax.fori_loop(CHUNKS - SLOTS, CHUNKS, body, 0)

            @pl.when(pos == DP - 1)
            def _():
                def body(c, carry):
                    total_copy(way, c, prv).wait_send()
                    keep_copy(way, c).wait()
                    return carry
                lax.fori_loop(CHUNKS - STAGES, CHUNKS, body, 0)

            @pl.when((pos > 0) & (pos < DP - 1))
            def _():
                def body(c, carry):
                    pass_copy(way, c, prv).wait_send()
                    return carry
                lax.fori_loop(0, CHUNKS, body, 0)

    def rows(i):
        return pl.ds(pl.multiple_of(i * BLK, BLK), BLK)

    def at(base, b):
        return pl.ds(pl.multiple_of(base + b * BLK, BLK), BLK)

    def hat(ref, rs, k):
        return (ref[rs, :].astype(F32) - st_ref[rs, k:k + 1]) * st_ref[rs, k + 1:k + 2]

    def norm_back(d_norm, x_hat, rstd, gain):
        scaled = d_norm * gain
        scaled_mean = jnp.mean(scaled, axis=-1, keepdims=True)
        proj_mean = jnp.mean(scaled * x_hat, axis=-1, keepdims=True)
        return rstd * (scaled - scaled_mean - x_hat * proj_mean)

    def gain(k):
        return gn_ref[k:k + 1, :].astype(F32)

    def mate_copy(rnd, b):
        return pltpu.make_async_remote_copy(
            src_ref=part.at[at(par0, b)], dst_ref=recv_a.at[b], send_sem=pa_send.at[rnd, b],
            recv_sem=pa_recv.at[rnd, b], device_id=mate, device_id_type=MESH)

    def peer_copy(rnd, b):
        dst = (recv_b, recv_c)[rnd]
        return pltpu.make_async_remote_copy(
            src_ref=part.at[at(own0, b)], dst_ref=dst.at[b], send_sem=pb_send.at[rnd, b],
            recv_sem=pb_recv.at[rnd, b], device_id=peer, device_id_type=MESH)

    def chip_sum(rnd, b):
        mate_copy(rnd, b).wait_recv()
        ro = at(own0, b)
        part[ro, :] = (part[ro, :].astype(F32) + recv_a[b].astype(F32)).astype(BF16)
        peer_copy(rnd, b).start()

    def part_block(rnd, b, fn):
        rp = at(par0, b)
        part[rp, :] = fn(rp).astype(BF16)
        mate_copy(rnd, b).start()
        ro = at(own0, b)
        part[ro, :] = fn(ro).astype(BF16)

    def mlp(act_s, da_s):
        def fwd(i, carry):
            rs = rows(i)
            n2 = (hat(h_ref, rs, 2) * gain(1)).astype(BF16)
            nrm[rs, :] = n2
            pre = dot_nn(n2, w1_ref[...]).astype(BF16).astype(F32)
            th = jnp.tanh(GELU_C * (pre + 0.044715 * pre * pre * pre))
            act_s[rs, :] = (0.5 * pre * (1.0 + th)).astype(BF16)
            slope = 0.5 * (1.0 + th) + 0.5 * pre * (1.0 - th * th) * GELU_C * (1.0 + 0.134145 * pre * pre)
            da_s[rs, :] = (dot_nt(dy_ref[rs, :], w2_ref[...]) * slope).astype(BF16)
            return carry
        lax.fori_loop(0, NBLK, fwd, 0)

        def down(j, carry):
            gb[rows(j), :] = dot_tn(act_s[:, rows(j)], dy_ref[...])
            pl.when(lax.rem(j, 2) == 1)(lambda: chain_step(lax.div(j, 2)))
            return carry
        lax.fori_loop(0, DIM // BLK, down, 0)

        def dn2(b, carry):
            part_block(0, b, lambda rs: dot_nt(da_s[rs, :], w1_ref[...]))
            pl.when(b > 0)(lambda: chip_sum(0, b - 1))
            chain_step(2 + b)
            return carry
        lax.fori_loop(0, HBLK, dn2, 0)
        chip_sum(0, HBLK - 1)

        def up(j, carry):
            gb[at(DIM, j), :] = dot_tn(nrm[:, rows(j)], da_s[...])
            pl.when(lax.rem(j, 2) == 1)(lambda: chain_step(5 + lax.div(j, 2)))
            return carry
        lax.fori_loop(0, DIM // BLK, up, 0)

    pl.run_scoped(mlp, pltpu.VMEM((TOK, DIM), BF16), pltpu.VMEM((TOK, DIM), BF16))

    def mid_copy(b):
        return pltpu.make_async_remote_copy(
            src_ref=dh_b.at[at(own0, b)], dst_ref=dh_b.at[at(own0, b)], send_sem=pd_send.at[0, b],
            recv_sem=pd_recv.at[0, b], device_id=mate, device_id_type=MESH)

    def out_copy(b):
        return pltpu.make_async_remote_copy(
            src_ref=part.at[at(own0, b)], dst_ref=dx_ref.at[at(own0, b)], send_sem=pd_send.at[1, b],
            recv_sem=pd_recv.at[1, b], device_id=mate, device_id_type=MESH)

    def out_keep(b):
        return pltpu.make_async_copy(part.at[at(own0, b)], dx_ref.at[at(own0, b)], dx_copy.at[b])

    def attention(qkv, d_qkv, o_s, do_s, acc_k, acc_v):
        def proj(i, carry):
            rs = rows(i)
            n1 = (hat(x_ref, rs, 0) * gain(0)).astype(BF16)
            nrm[rs, :] = n1
            qkv[rs, :] = dot_nt(n1, wq_ref[...]).astype(BF16)
            pl.when(lax.rem(i, 2) == 1)(lambda: chain_step(7 + lax.div(i, 2)))
            return carry
        lax.fori_loop(0, NBLK, proj, 0)

        def mid(b, carry):
            chain_step(10 + 2 * b)
            chain_step(11 + 2 * b)
            peer_copy(0, b).wait_recv()
            ro = at(own0, b)
            d_norm = part[ro, :].astype(F32) + recv_b[b].astype(F32)
            dh = dy_ref[ro, :].astype(F32) + norm_back(d_norm, hat(h_ref, ro, 2), st_ref[ro, 3:4], gain(1))
            dh_f[rows(b), :] = dh
            dh_b[ro, :] = dh.astype(BF16)
            mid_copy(b).start()
            return carry
        lax.fori_loop(0, HBLK, mid, 0)
        for b in range(HBLK):
            mid_copy(b).wait_recv()

        def d_out(i, carry):
            do_s[rows(i), :] = dot_nt(dh_b[rows(i), :], wo_ref[...]).astype(BF16)
            return carry
        lax.fori_loop(0, NBLK, d_out, 0)

        lane = lax.broadcasted_iota(jnp.int32, (BLK, 128), 1)
        causal = lax.broadcasted_iota(jnp.int32, (BLK, BLK), 1) <= lax.broadcasted_iota(jnp.int32, (BLK, BLK), 0)
        zero = jnp.zeros((BLK, 128), BF16)

        def pair(p, carry):
            def cols(k):
                return pl.ds(pl.multiple_of(k * 256 + p * 128, 128), 128)
            for n, i in enumerate(reversed(range(NBLK))):
                span = (i + 1) * BLK
                rs = slice(i * BLK, span)
                k_all = qkv[0:span, cols(1)]
                v_all = qkv[0:span, cols(2)]
                outs, dqs = [], []
                dk = dv = None
                for hh in (0, 1):
                    mine = (lane < 64) if hh == 0 else (lane >= 64)
                    q = jnp.where(mine, qkv[rs, cols(0)], zero)
                    do = jnp.where(mine, do_s[rs, cols(0)], zero)
                    sc = dot_nt(q, k_all) * 0.125
                    last = jnp.where(causal, sc[:, span - BLK:], -1e30)
                    sc = jnp.concatenate([sc[:, :span - BLK], last], axis=1) if i else last
                    ex = jnp.exp(sc - jnp.max(sc, axis=-1, keepdims=True))
                    prob = ex * (1.0 / jnp.sum(ex, axis=-1, keepdims=True))
                    prob_lo = prob.astype(BF16)
                    outs.append(dot_nn(prob_lo, v_all))
                    dp = dot_nt(do, v_all)
                    ds = (prob * (dp - jnp.sum(prob * dp, axis=-1, keepdims=True)) * 0.125).astype(BF16)
                    dqs.append(dot_nn(ds, k_all))
                    dv_h = dot_tn(prob_lo, do)
                    dk_h = dot_tn(ds, q)
                    if i == NBLK - 1 and hh == 0:
                        acc_v[...] = dv_h
                        acc_k[...] = dk_h
                    else:
                        acc_v[0:span, :] += dv_h
                        acc_k[0:span, :] += dk_h
                o_s[rs, cols(0)] = jnp.where(lane < 64, outs[0], outs[1]).astype(BF16)
                d_qkv[rs, cols(0)] = jnp.where(lane < 64, dqs[0], dqs[1]).astype(BF16)
                chain_step(16 + p * NBLK + n)
            d_qkv[:, cols(1)] = acc_k[...].astype(BF16)
            d_qkv[:, cols(2)] = acc_v[...].astype(BF16)
            return carry
        lax.fori_loop(0, 2, pair, 0)

        gb[2 * DIM:2 * DIM + BLK, :] = dot_tn(o_s[...], dh_b[...])
        chain_step(28)

        def w_qkv(j, carry):
            gb[at(2 * DIM + BLK, j), :] = dot_tn(d_qkv[:, rows(j)], nrm[...])
            chain_step(29 + j)
            return carry
        lax.fori_loop(0, 3, w_qkv, 0)

        for b in range(HBLK):
            mate_copy(0, b).wait_send()
            peer_copy(0, b).wait_send()
            mid_copy(b).wait_send()

        def dn1(b, carry):
            part_block(1, b, lambda rs: dot_nn(d_qkv[rs, :], wq_ref[...]))
            pl.when(b > 0)(lambda: chip_sum(1, b - 1))
            chain_step(32 + b)
            return carry
        lax.fori_loop(0, HBLK, dn1, 0)
        chip_sum(1, HBLK - 1)

    pl.run_scoped(attention, pltpu.VMEM((TOK, 768), BF16), pltpu.VMEM((TOK, 768), BF16),
                  pltpu.VMEM((TOK, BLK), BF16), pltpu.VMEM((TOK, BLK), BF16),
                  pltpu.VMEM((TOK, 128), F32), pltpu.VMEM((TOK, 128), F32))

    def final(b, carry):
        chain_step(35 + 3 * b)
        chain_step(36 + 3 * b)
        chain_step(37 + 3 * b)
        peer_copy(1, b).wait_recv()
        peer_copy(1, b).wait_send()
        ro = at(own0, b)
        d_norm = part[ro, :].astype(F32) + recv_c[b].astype(F32)
        dx = dh_f[rows(b), :] + norm_back(d_norm, hat(x_ref, ro, 0), st_ref[ro, 1:2], gain(0))
        part[ro, :] = dx.astype(BF16)
        out_copy(b).start()
        out_keep(b).start()
        return carry
    lax.fori_loop(0, HBLK, final, 0)
    chain_steps(35 + 3 * HBLK, STEPS - 35 - 3 * HBLK)
    chain_end()
    for b in range(HBLK):
        mate_copy(1, b).wait_send()
        out_copy(b).wait()
        out_keep(b).wait()


def solution(mesh):
    row_spec = P(('pod', 'dp'), None)
    stat_spec = P(('pod', 'dp'))
    in_specs = (row_spec, row_spec, stat_spec, stat_spec, stat_spec, stat_spec, P(None), P(None), row_spec,
                P(None, None, 'tp', None), P('tp', None, None), P(None, 'tp'), P('tp', None))
    out_specs = (row_spec, P('pod', None, 'tp', None), P(('pod', 'tp'), None, None), P('pod', 'tp'), P(('pod', 'tp'), None))

    vmem = pl.BlockSpec(memory_space=pltpu.VMEM)
    hbm = pl.BlockSpec(memory_space=pl.ANY)
    dma = pltpu.SemaphoreType.DMA
    scratch = [
        pltpu.VMEM((ROWS, DIM), F32),
        pltpu.VMEM((2, SLOTS, CROWS, DIM), F32),
        pltpu.VMEM((2, STAGES, CROWS, DIM), BF16),
        pltpu.VMEM((TOK, DIM), BF16),
        pltpu.VMEM((TOK, DIM), BF16),
        pltpu.VMEM((HBLK, BLK, DIM), BF16),
        pltpu.VMEM((HBLK, BLK, DIM), BF16),
        pltpu.VMEM((HBLK, BLK, DIM), BF16),
        pltpu.VMEM((HALF, DIM), F32),
        pltpu.VMEM((TOK, DIM), BF16),
        dma((2, SLOTS)), dma((2, SLOTS)), pltpu.SemaphoreType.REGULAR((2,)),
        dma((2, CHUNKS)), dma((2, CHUNKS)), dma((2, STAGES)),
        dma((2, HBLK)), dma((2, HBLK)), dma((2, HBLK)), dma((2, HBLK)),
        dma((2, HBLK)), dma((2, HBLK)), dma((HBLK,)),
    ]
    layer = pl.pallas_call(
        layer_kernel,
        out_shape=(jax.ShapeDtypeStruct((TOK, DIM), BF16), jax.ShapeDtypeStruct((ROWS, DIM), BF16)),
        in_specs=[vmem] * 9,
        out_specs=(hbm, hbm),
        scratch_shapes=scratch,
        compiler_params=pltpu.CompilerParams(collective_id=0, has_side_effects=True, vmem_limit_bytes=67043328),
        name='layer_backward')

    def local_step(x_saved, h_saved, mean_one, rstd_one, mean_two, rstd_two, gain_one, gain_two, grad_y, w_qkv, w_proj, w_up, w_down):
        stats = jnp.stack([mean_one, rstd_one, mean_two, rstd_two], axis=1)
        gains = jnp.stack([gain_one, gain_two], axis=0)
        wq_t = jnp.transpose(w_qkv, (1, 2, 3, 0)).reshape(768, DIM)
        grad_x, grads = layer(x_saved, h_saved, grad_y, stats, gains, wq_t, w_proj.reshape(BLK, DIM), w_up, w_down)
        grad_qkv = jnp.transpose(grads[2 * DIM + BLK:].reshape(3, 4, 64, DIM), (3, 0, 1, 2))
        return (grad_x, grad_qkv, grads[2 * DIM:2 * DIM + BLK].reshape(4, 64, DIM), grads[DIM:2 * DIM], grads[:DIM])

    return jax.shard_map(local_step, mesh=mesh, in_specs=in_specs, out_specs=out_specs, check_vma=False)
```

```python
import functools
import math
import jax
import jax.numpy as jnp
from jax import lax
from jax.experimental import pallas as pl
from jax.experimental.pallas import tpu as pltpu
from jax.sharding import PartitionSpec as P

GELU_C = math.sqrt(2.0 / math.pi)
MESH = pl.DeviceIdType.MESH
F32 = jnp.float32
BF16 = jnp.bfloat16

TOK = 1536
DIM = 1024
BLK = 256
HALF = TOK // 2
NBLK = TOK // BLK
HBLK = HALF // BLK
CROWS = 32
ROWS = 3072
CHUNKS = ROWS // (2 * CROWS)
SLOTS = 16
LAG = 2
DP = 4
OUT_SPACE = pltpu.VMEM
VMEM_LIMIT = 54 * 2 ** 20
STEPS = CHUNKS + 2 * LAG * (DP - 1)


def dot_nn(a, b):
    return lax.dot_general(a, b, (((1,), (0,)), ((), ())), preferred_element_type=F32)


def dot_nt(a, b):
    return lax.dot_general(a, b, (((1,), (1,)), ((), ())), preferred_element_type=F32)


def dot_tn(a, b):
    return lax.dot_general(a, b, (((0,), (0,)), ((), ())), preferred_element_type=F32)


def layer_kernel(x_hbm, h_hbm, dy_hbm, m1_ref, r1_ref, m2_ref, r2_ref, g1_ref, g2_ref, wq_hbm, wo_hbm, w1_hbm, w2_hbm,
                 part, fb_ref,
                 gb, land, nrm, recv_a, recv_b, recv_c, dh_f, dh_b, h_ref, dy_ref, st_ref, gn_ref,
                 ch_send, ch_recv, ch_free, fb_send, fb_recv,
                 pa_send, pa_recv, pb_send, pb_recv, pd_send, pd_recv, in_sem, mate_done):
    pod, z, tp = lax.axis_index('pod'), lax.axis_index('dp'), lax.axis_index('tp')
    core = lax.rem(tp, 2)
    mate = (pod, z, tp + 1 - 2 * core)
    peer = (pod, z, lax.rem(tp + 2, 4))
    z_hi = jnp.minimum(z + 1, DP - 1)
    z_lo = jnp.maximum(z - 1, 0)
    own0 = core * HALF
    par0 = HALF - own0

    def rows(i):
        return pl.ds(pl.multiple_of(i * BLK, BLK), BLK)

    def at(base, b):
        return pl.ds(pl.multiple_of(base + b * BLK, BLK), BLK)

    def h_copy(i):
        return pltpu.make_async_copy(h_hbm.at[rows(i)], h_ref.at[rows(i)], in_sem.at[i])

    dy_copy = pltpu.make_async_copy(dy_hbm, dy_ref, in_sem.at[6])
    for i in range(NBLK):
        h_copy(i).start()

    barrier = pltpu.get_barrier_semaphore()
    for dev in (mate, peer):
        pl.semaphore_signal(barrier, inc=1, device_id=dev, device_id_type=MESH)
    pl.when(z < DP - 1)(lambda: pl.semaphore_signal(barrier, inc=1, device_id=(pod, z_hi, tp), device_id_type=MESH))
    pl.when(z > 0)(lambda: pl.semaphore_signal(barrier, inc=1, device_id=(pod, z_lo, tp), device_id_type=MESH))
    pl.semaphore_wait(barrier, 2 + jnp.where(z < DP - 1, 1, 0) + jnp.where(z > 0, 1, 0))

    def way_of(way):
        if way == 0:
            return z, (pod, z_hi, tp), (pod, z_lo, tp)
        return DP - 1 - z, (pod, z_lo, tp), (pod, z_hi, tp)

    def rows_of(way, c):
        return pl.ds(pl.multiple_of(c * (2 * CROWS) + way * CROWS, CROWS), CROWS)

    def chain_copy(way, c, nxt):
        slot = lax.rem(c, SLOTS)
        return pltpu.make_async_remote_copy(
            src_ref=gb.at[rows_of(way, c)], dst_ref=land.at[way, slot], send_sem=ch_send.at[way, slot],
            recv_sem=ch_recv.at[way, slot], device_id=nxt, device_id_type=MESH)

    def pass_copy(way, c, prv):
        return pltpu.make_async_remote_copy(
            src_ref=fb_ref.at[rows_of(way, c)], dst_ref=fb_ref.at[rows_of(way, c)], send_sem=fb_send.at[way, c],
            recv_sem=fb_recv.at[way, c], device_id=prv, device_id_type=MESH)

    def chain_step(s):
        for way in (0, 1):
            pos, nxt, prv = way_of(way)
            c = s - LAG * pos

            @pl.when((c >= 0) & (c < CHUNKS))
            def _():
                @pl.when(pos > 0)
                def _():
                    chain_copy(way, c, nxt).wait_recv()
                    gb[rows_of(way, c), :] += land[way, lax.rem(c, SLOTS)]

                    @pl.when(c < CHUNKS - SLOTS)
                    def _():
                        pl.semaphore_signal(ch_free.at[way], inc=1, device_id=prv, device_id_type=MESH)

                @pl.when(pos < DP - 1)
                def _():
                    @pl.when(c >= SLOTS)
                    def _():
                        pl.semaphore_wait(ch_free.at[way], 1)
                        chain_copy(way, c - SLOTS, nxt).wait_send()
                    chain_copy(way, c, nxt).start()

                @pl.when(pos == DP - 1)
                def _():
                    fb_ref[rows_of(way, c), :] = gb[rows_of(way, c), :].astype(BF16)
                    pass_copy(way, c, prv).start()

            c2 = s - LAG * (2 * (DP - 1) - pos)

            @pl.when((pos < DP - 1) & (c2 >= 0) & (c2 < CHUNKS))
            def _():
                pass_copy(way, c2, prv).wait_recv()

                @pl.when(pos > 0)
                def _():
                    pass_copy(way, c2, prv).start()

    def chain_steps(s0, n):
        def body(k, carry):
            chain_step(s0 + k)
            return carry
        lax.fori_loop(0, n, body, 0)

    def chain_end():
        for way in (0, 1):
            pos, nxt, prv = way_of(way)

            @pl.when(pos < DP - 1)
            def _():
                def body(c, carry):
                    chain_copy(way, c, nxt).wait_send()
                    return carry
                lax.fori_loop(CHUNKS - SLOTS, CHUNKS, body, 0)

            @pl.when(pos > 0)
            def _():
                def body(c, carry):
                    pass_copy(way, c, prv).wait_send()
                    return carry
                lax.fori_loop(0, CHUNKS, body, 0)

    def hat(ref, rs, k):
        return (ref[rs, :].astype(F32) - st_ref[rs, k:k + 1]) * st_ref[rs, k + 1:k + 2]

    def norm_back(d_norm, x_hat, rstd, gain):
        scaled = d_norm * gain
        scaled_mean = jnp.mean(scaled, axis=-1, keepdims=True)
        proj_mean = jnp.mean(scaled * x_hat, axis=-1, keepdims=True)
        return rstd * (scaled - scaled_mean - x_hat * proj_mean)

    def gain(k):
        return gn_ref[k:k + 1, :]

    def put_stats(k, ref):
        stat_t = jnp.transpose(ref[...])
        for b in range(TOK // 128):
            st_ref[b * 128:(b + 1) * 128, k:k + 1] = stat_t[:, b:b + 1]

    def put_gain(k, ref):
        wide = ref[...].astype(F32)
        for b in range(8):
            gn_ref[k:k + 1, b * 128:(b + 1) * 128] = wide[b:b + 1, :]

    def mate_copy(rnd, b):
        return pltpu.make_async_remote_copy(
            src_ref=part.at[at(par0, b)], dst_ref=recv_a.at[b], send_sem=pa_send.at[rnd, b],
            recv_sem=pa_recv.at[rnd, b], device_id=mate, device_id_type=MESH)

    def peer_copy(rnd, b):
        dst = (recv_b, recv_c)[rnd]
        return pltpu.make_async_remote_copy(
            src_ref=part.at[at(own0, b)], dst_ref=dst.at[b], send_sem=pb_send.at[rnd, b],
            recv_sem=pb_recv.at[rnd, b], device_id=peer, device_id_type=MESH)

    def chip_sum(rnd, b):
        mate_copy(rnd, b).wait_recv()
        ro = at(own0, b)
        part[ro, :] = (part[ro, :].astype(F32) + recv_a[b].astype(F32)).astype(BF16)
        peer_copy(rnd, b).start()

    def part_block(rnd, b, fn):
        rp = at(par0, b)
        part[rp, :] = fn(rp).astype(BF16)
        mate_copy(rnd, b).start()
        ro = at(own0, b)
        part[ro, :] = fn(ro).astype(BF16)

    def mlp(w1_ref, w2_ref, act_s, da_s):
        def w1_copy(j):
            return pltpu.make_async_copy(w1_hbm.at[:, rows(j)], w1_ref.at[:, rows(j)], in_sem.at[7 + j])

        def w2_copy(j):
            return pltpu.make_async_copy(w2_hbm.at[rows(j)], w2_ref.at[rows(j)], in_sem.at[11 + j])

        w1_copy(0).start()
        w2_copy(0).start()
        dy_copy.start()
        for j in range(1, 4):
            w1_copy(j).start()
            w2_copy(j).start()
        put_stats(2, m2_ref)
        put_stats(3, r2_ref)
        put_gain(1, g2_ref)

        def norm_two(i, carry):
            h_copy(i).wait()
            nrm[rows(i), :] = (hat(h_ref, rows(i), 2) * gain(1)).astype(BF16)
            return carry
        lax.fori_loop(0, NBLK, norm_two, 0)

        def column(j, carry):
            w1_copy(j).wait()
            w2_copy(j).wait()
            pl.when(j == 0)(lambda: dy_copy.wait())

            def fwd(i, carry):
                rs = pl.ds(pl.multiple_of(i * 512, 512), 512)
                pre = dot_nn(nrm[rs, :], w1_ref[:, rows(j)]).astype(BF16).astype(F32)
                th = jnp.tanh(GELU_C * (pre + 0.044715 * pre * pre * pre))
                act_s[rs, :] = (0.5 * pre * (1.0 + th)).astype(BF16)
                slope = 0.5 * (1.0 + th) + 0.5 * pre * (1.0 - th * th) * GELU_C * (1.0 + 0.134145 * pre * pre)
                da_s[rs, rows(j)] = (dot_nt(dy_ref[rs, :], w2_ref[rows(j), :]) * slope).astype(BF16)
                pl.when((i == 1) & (j > 0))(lambda: chain_step(2 * j - 1))
                return carry
            lax.fori_loop(0, 3, fwd, 0)
            gb[rows(j), :] = dot_tn(act_s[...], dy_ref[...])
            chain_step(2 * j)
            return carry
        lax.fori_loop(0, DIM // BLK, column, 0)

        def dn2(b, carry):
            part_block(0, b, lambda rs: dot_nt(da_s[rs, :], w1_ref[...]))
            pl.when(b > 0)(lambda: chip_sum(0, b - 1))
            chain_step(7 + b)
            return carry
        lax.fori_loop(0, HBLK, dn2, 0)
        chip_sum(0, HBLK - 1)

        def up(j, carry):
            gb[at(DIM, j), :] = dot_tn(nrm[:, rows(j)], da_s[...])
            pl.when(lax.rem(j, 2) == 1)(lambda: chain_step(10 + lax.div(j, 2)))
            return carry
        lax.fori_loop(0, DIM // BLK, up, 0)

    pl.run_scoped(mlp, pltpu.VMEM((DIM, DIM), BF16), pltpu.VMEM((DIM, DIM), BF16),
                  pltpu.VMEM((TOK, BLK), BF16), pltpu.VMEM((TOK, DIM), BF16))
    put_stats(0, m1_ref)
    put_stats(1, r1_ref)
    put_gain(0, g1_ref)

    def mid_copy(b):
        return pltpu.make_async_remote_copy(
            src_ref=dh_b.at[at(own0, b)], dst_ref=dh_b.at[at(own0, b)], send_sem=pd_send.at[0, b],
            recv_sem=pd_recv.at[0, b], device_id=mate, device_id_type=MESH)

    def out_copy(b):
        return pltpu.make_async_remote_copy(
            src_ref=part.at[at(own0, b)], dst_ref=part.at[at(own0, b)], send_sem=pd_send.at[1, b],
            recv_sem=pd_recv.at[1, b], device_id=mate, device_id_type=MESH)

    def attention(x_ref, wq_ref, wo_ref, qkv, d_qkv, o_s, do_s, acc_k, acc_v):
        x_copy = pltpu.make_async_copy(x_hbm, x_ref, in_sem.at[15])
        wq_copy = pltpu.make_async_copy(wq_hbm, wq_ref, in_sem.at[16])
        wo_copy = pltpu.make_async_copy(wo_hbm, wo_ref, in_sem.at[17])
        x_copy.start()
        wq_copy.start()
        wo_copy.start()
        x_copy.wait()
        wq_copy.wait()
        wo_copy.wait()

        def proj(i, carry):
            rs = rows(i)
            n1 = (hat(x_ref, rs, 0) * gain(0)).astype(BF16)
            nrm[rs, :] = n1
            qkv[rs, :] = dot_nt(n1, wq_ref[...]).astype(BF16)
            pl.when(lax.rem(i, 2) == 1)(lambda: chain_step(12 + lax.div(i, 2)))
            return carry
        lax.fori_loop(0, NBLK, proj, 0)

        def mid(b, carry):
            chain_step(15 + b)
            peer_copy(0, b).wait_recv()
            ro = at(own0, b)
            d_norm = part[ro, :].astype(F32) + recv_b[b].astype(F32)
            dh = dy_ref[ro, :].astype(F32) + norm_back(d_norm, hat(h_ref, ro, 2), st_ref[ro, 3:4], gain(1))
            dh_f[rows(b), :] = dh
            dh_b[ro, :] = dh.astype(BF16)
            mid_copy(b).start()
            return carry
        lax.fori_loop(0, HBLK, mid, 0)
        for b in range(HBLK):
            mid_copy(b).wait_recv()

        def d_out(i, carry):
            do_s[rows(i), :] = dot_nt(dh_b[rows(i), :], wo_ref[...]).astype(BF16)
            return carry
        lax.fori_loop(0, NBLK, d_out, 0)

        lane = lax.broadcasted_iota(jnp.int32, (BLK, 128), 1)
        causal = lax.broadcasted_iota(jnp.int32, (BLK, BLK), 1) <= lax.broadcasted_iota(jnp.int32, (BLK, BLK), 0)
        zero = jnp.zeros((BLK, 128), BF16)

        def pair(p, carry):
            def cols(k):
                return pl.ds(pl.multiple_of(k * 256 + p * 128, 128), 128)
            for n, i in enumerate(reversed(range(NBLK))):
                span = (i + 1) * BLK
                rs = slice(i * BLK, span)
                k_all = qkv[0:span, cols(1)]
                v_all = qkv[0:span, cols(2)]
                outs, dqs = [], []
                dk = dv = None
                for hh in (0, 1):
                    mine = (lane < 64) if hh == 0 else (lane >= 64)
                    q = jnp.where(mine, qkv[rs, cols(0)], zero)
                    do = jnp.where(mine, do_s[rs, cols(0)], zero)
                    sc = dot_nt(q, k_all) * 0.125
                    last = jnp.where(causal, sc[:, span - BLK:], -1e30)
                    sc = jnp.concatenate([sc[:, :span - BLK], last], axis=1) if i else last
                    ex = jnp.exp(sc - jnp.max(sc, axis=-1, keepdims=True))
                    prob = ex * (1.0 / jnp.sum(ex, axis=-1, keepdims=True))
                    prob_lo = prob.astype(BF16)
                    outs.append(dot_nn(prob_lo, v_all))
                    dp = dot_nt(do, v_all)
                    ds = (prob * (dp - jnp.sum(prob * dp, axis=-1, keepdims=True)) * 0.125).astype(BF16)
                    dqs.append(dot_nn(ds, k_all))
                    dv_h = dot_tn(prob_lo, do)
                    dk_h = dot_tn(ds, q)
                    if i == NBLK - 1 and hh == 0:
                        acc_v[...] = dv_h
                        acc_k[...] = dk_h
                    else:
                        acc_v[0:span, :] += dv_h
                        acc_k[0:span, :] += dk_h
                o_s[rs, cols(0)] = jnp.where(lane < 64, outs[0], outs[1]).astype(BF16)
                d_qkv[rs, cols(0)] = jnp.where(lane < 64, dqs[0], dqs[1]).astype(BF16)
                chain_step(18 + p * NBLK + n)
            d_qkv[:, cols(1)] = acc_k[...].astype(BF16)
            d_qkv[:, cols(2)] = acc_v[...].astype(BF16)
            return carry
        lax.fori_loop(0, 2, pair, 0)

        gb[2 * DIM:2 * DIM + BLK, :] = dot_tn(o_s[...], dh_b[...])
        chain_step(30)

        def w_qkv(j, carry):
            gb[at(2 * DIM + BLK, j), :] = dot_tn(d_qkv[:, rows(j)], nrm[...])
            chain_step(31 + j)
            return carry
        lax.fori_loop(0, 3, w_qkv, 0)

        for b in range(HBLK):
            mate_copy(0, b).wait_send()
            peer_copy(0, b).wait_send()
            mid_copy(b).wait_send()

        def dn1(b, carry):
            part_block(1, b, lambda rs: dot_nn(d_qkv[rs, :], wq_ref[...]))
            pl.when(b > 0)(lambda: chip_sum(1, b - 1))
            chain_step(34 + b)
            return carry
        lax.fori_loop(0, HBLK, dn1, 0)
        chip_sum(1, HBLK - 1)

        def final(b, carry):
            chain_step(37 + 3 * b)
            chain_step(38 + 3 * b)
            chain_step(39 + 3 * b)
            peer_copy(1, b).wait_recv()
            peer_copy(1, b).wait_send()
            ro = at(own0, b)
            d_norm = part[ro, :].astype(F32) + recv_c[b].astype(F32)
            dx = dh_f[rows(b), :] + norm_back(d_norm, hat(x_ref, ro, 0), st_ref[ro, 1:2], gain(0))
            part[ro, :] = dx.astype(BF16)
            out_copy(b).start()
            return carry
        for b in range(HBLK):
            mate_copy(1, b).wait_send()
        pl.semaphore_signal(mate_done, inc=1, device_id=mate, device_id_type=MESH)
        pl.semaphore_wait(mate_done, 1)
        lax.fori_loop(0, HBLK, final, 0)

    pl.run_scoped(attention, pltpu.VMEM((TOK, DIM), BF16), pltpu.VMEM((768, DIM), BF16), pltpu.VMEM((BLK, DIM), BF16),
                  pltpu.VMEM((TOK, 768), BF16), pltpu.VMEM((TOK, 768), BF16),
                  pltpu.VMEM((TOK, BLK), BF16), pltpu.VMEM((TOK, BLK), BF16),
                  pltpu.VMEM((TOK, 128), F32), pltpu.VMEM((TOK, 128), F32))

    chain_steps(37 + 3 * HBLK, STEPS - 37 - 3 * HBLK)
    chain_end()
    for b in range(HBLK):
        out_copy(b).wait()


def solution(mesh):
    row_spec = P(('pod', 'dp'), None)
    stat_spec = P(('pod', 'dp'))
    in_specs = (row_spec, row_spec, stat_spec, stat_spec, stat_spec, stat_spec, P(None), P(None), row_spec,
                P(None, None, 'tp', None), P('tp', None, None), P(None, 'tp'), P('tp', None))
    out_specs = (row_spec, P('pod', None, 'tp', None), P(('pod', 'tp'), None, None), P('pod', 'tp'), P(('pod', 'tp'), None))

    vmem = pl.BlockSpec(memory_space=pltpu.VMEM)
    hbm = pl.BlockSpec(memory_space=pl.ANY)
    dma = pltpu.SemaphoreType.DMA
    scratch = [
        pltpu.VMEM((ROWS, DIM), F32),
        pltpu.VMEM((2, SLOTS, CROWS, DIM), F32),
        pltpu.VMEM((TOK, DIM), BF16),
        pltpu.VMEM((HBLK, BLK, DIM), BF16),
        pltpu.VMEM((HBLK, BLK, DIM), BF16),
        pltpu.VMEM((HBLK, BLK, DIM), BF16),
        pltpu.VMEM((HALF, DIM), F32),
        pltpu.VMEM((TOK, DIM), BF16),
        pltpu.VMEM((TOK, DIM), BF16),
        pltpu.VMEM((TOK, DIM), BF16),
        pltpu.VMEM((TOK, 4), F32),
        pltpu.VMEM((2, DIM), F32),
        dma((2, SLOTS)), dma((2, SLOTS)), pltpu.SemaphoreType.REGULAR((2,)),
        dma((2, CHUNKS)), dma((2, CHUNKS)),
        dma((2, HBLK)), dma((2, HBLK)), dma((2, HBLK)), dma((2, HBLK)),
        dma((2, HBLK)), dma((2, HBLK)), dma((18,)), pltpu.SemaphoreType.REGULAR,
    ]
    layer = pl.pallas_call(
        layer_kernel,
        out_shape=(OUT_SPACE((TOK, DIM), BF16), OUT_SPACE((ROWS, DIM), BF16)),
        in_specs=[hbm] * 3 + [vmem] * 6 + [hbm] * 4,
        out_specs=(vmem, vmem),
        scratch_shapes=scratch,
        compiler_params=pltpu.CompilerParams(collective_id=0, has_side_effects=True, vmem_limit_bytes=VMEM_LIMIT),
        name='layer_backward')

    def local_step(x_saved, h_saved, mean_one, rstd_one, mean_two, rstd_two, gain_one, gain_two, grad_y, w_qkv, w_proj, w_up, w_down):
        small = [a.reshape(-1, 128) for a in (mean_one, rstd_one, mean_two, rstd_two, gain_one, gain_two)]
        wq_t = jnp.transpose(w_qkv, (1, 2, 3, 0)).reshape(768, DIM)
        grad_x, grads = layer(x_saved, h_saved, grad_y, *small, wq_t, w_proj.reshape(BLK, DIM), w_up, w_down)
        grad_qkv = jnp.transpose(grads[2 * DIM + BLK:].reshape(3, 4, 64, DIM), (3, 0, 1, 2))
        return (grad_x, grad_qkv, grads[2 * DIM:2 * DIM + BLK].reshape(4, 64, DIM), grads[DIM:2 * DIM], grads[:DIM])

    return jax.shard_map(local_step, mesh=mesh, in_specs=in_specs, out_specs=out_specs, check_vma=False)
```

```python
import functools
import math
import jax
import jax.numpy as jnp
from jax import lax
from jax.experimental import pallas as pl
from jax.experimental.pallas import tpu as pltpu
from jax.sharding import PartitionSpec as P

GELU_C = math.sqrt(2.0 / math.pi)
MESH = pl.DeviceIdType.MESH
F32 = jnp.float32
BF16 = jnp.bfloat16

TOK = 1536
DIM = 1024
BLK = 256
HALF = TOK // 2
NBLK = TOK // BLK
HBLK = HALF // BLK
CROWS = 32
SROWS = 16
SMALL = 8
ROWS = 3072
CHUNKS = SMALL + (ROWS - 2 * SROWS * SMALL) // (2 * CROWS)
SLOTS = 8
LAG = 2
LAG_BACK = 3
HOLD = 0
DP = 4
OUT_SPACE = pltpu.VMEM
VMEM_LIMIT = 54 * 2 ** 20
CLOSE_LIMIT = 1 * 2 ** 20
STEPS = CHUNKS + (LAG + LAG_BACK) * (DP - 1) + HOLD


def dot_nn(a, b):
    return lax.dot_general(a, b, (((1,), (0,)), ((), ())), preferred_element_type=F32)


def dot_nt(a, b):
    return lax.dot_general(a, b, (((1,), (1,)), ((), ())), preferred_element_type=F32)


def dot_tn(a, b):
    return lax.dot_general(a, b, (((0,), (0,)), ((), ())), preferred_element_type=F32)


def layer_kernel(x_hbm, h_hbm, dy_hbm, m1_ref, r1_ref, m2_ref, r2_ref, g1_ref, g2_ref, wq_hbm, wo_hbm, w1_hbm, w2_hbm,
                 part, fb_ref,
                 gb, land, nrm, recv_a, recv_b, recv_c, dh_f, dh_b, h_ref, dy_ref, st_ref, gn_ref,
                 ch_send, ch_recv, ch_free, fb_send, fb_recv,
                 pa_send, pa_recv, pb_send, pb_recv, pd_send, pd_recv, in_sem, mate_done):
    pod, z, tp = lax.axis_index('pod'), lax.axis_index('dp'), lax.axis_index('tp')
    core = lax.rem(tp, 2)
    mate = (pod, z, tp + 1 - 2 * core)
    peer = (pod, z, lax.rem(tp + 2, 4))
    z_hi = jnp.minimum(z + 1, DP - 1)
    z_lo = jnp.maximum(z - 1, 0)
    own0 = core * HALF
    par0 = HALF - own0

    def rows(i):
        return pl.ds(pl.multiple_of(i * BLK, BLK), BLK)

    def at(base, b):
        return pl.ds(pl.multiple_of(base + b * BLK, BLK), BLK)

    def h_copy(i):
        return pltpu.make_async_copy(h_hbm.at[rows(i)], h_ref.at[rows(i)], in_sem.at[i])

    def dy_copy(i):
        return pltpu.make_async_copy(dy_hbm.at[rows(i)], dy_ref.at[rows(i)], in_sem.at[18 + i])

    barrier = pltpu.get_barrier_semaphore()
    for dev in (mate, peer):
        pl.semaphore_signal(barrier, inc=1, device_id=dev, device_id_type=MESH)
    pl.when(z < DP - 1)(lambda: pl.semaphore_signal(barrier, inc=1, device_id=(pod, z_hi, tp), device_id_type=MESH))
    pl.when(z > 0)(lambda: pl.semaphore_signal(barrier, inc=1, device_id=(pod, z_lo, tp), device_id_type=MESH))
    peers = 2 + jnp.where(z < DP - 1, 1, 0) + jnp.where(z > 0, 1, 0)

    def way_of(way):
        if way == 0:
            return z, (pod, z_hi, tp), (pod, z_lo, tp)
        return DP - 1 - z, (pod, z_lo, tp), (pod, z_hi, tp)

    def rows_of(way, c, big):
        if big:
            start = 2 * SROWS * SMALL + (c - SMALL) * (2 * CROWS) + way * CROWS
            return pl.ds(pl.multiple_of(start, CROWS), CROWS)
        return pl.ds(pl.multiple_of(c * (2 * SROWS) + way * SROWS, SROWS), SROWS)

    def land_at(way, c, big):
        return land.at[way, lax.rem(c, SLOTS), pl.ds(0, CROWS if big else SROWS)]

    def chain_copy(way, c, nxt, big):
        slot = lax.rem(c, SLOTS)
        return pltpu.make_async_remote_copy(
            src_ref=gb.at[rows_of(way, c, big)], dst_ref=land_at(way, c, big), send_sem=ch_send.at[way, slot],
            recv_sem=ch_recv.at[way, slot], device_id=nxt, device_id_type=MESH)

    def pass_copy(way, c, prv, big):
        return pltpu.make_async_remote_copy(
            src_ref=fb_ref.at[rows_of(way, c, big)], dst_ref=fb_ref.at[rows_of(way, c, big)], send_sem=fb_send.at[way, c],
            recv_sem=fb_recv.at[way, c], device_id=prv, device_id_type=MESH)

    def chain_step(s, early=False):
        for way in (0, 1):
            pos, nxt, prv = way_of(way)
            c = s - LAG * pos

            def reduce_step(big):
                rs = rows_of(way, c, big)

                @pl.when(pos > 0)
                def _():
                    chain_copy(way, c, nxt, big).wait_recv()
                    total = gb[rs, :] + land_at(way, c, big)[...]

                    @pl.when(pos < DP - 1)
                    def _():
                        gb[rs, :] = total

                    @pl.when(pos == DP - 1)
                    def _():
                        fb_ref[rs, :] = total.astype(BF16)

                    @pl.when(c < CHUNKS - SLOTS)
                    def _():
                        pl.semaphore_signal(ch_free.at[way], inc=1, device_id=prv, device_id_type=MESH)

                @pl.when(pos < DP - 1)
                def _():
                    @pl.when(c >= SLOTS)
                    def _():
                        pl.semaphore_wait(ch_free.at[way], 1)
                    pl.when((c >= SLOTS) & (c < SLOTS + SMALL))(lambda: chain_copy(way, c - SLOTS, nxt, False).wait_send())
                    pl.when(c >= SLOTS + SMALL)(lambda: chain_copy(way, c - SLOTS, nxt, True).wait_send())
                    chain_copy(way, c, nxt, big).start()

            if early:
                pl.when((c >= 0) & (c < SMALL))(lambda: reduce_step(False))
            pl.when((c >= SMALL) & (c < CHUNKS))(lambda: reduce_step(True))

            c2 = s - HOLD - LAG * (DP - 1) - LAG_BACK * (DP - 1 - pos)

            def pass_step(big):
                pl.when(pos < DP - 1)(lambda: pass_copy(way, c2, prv, big).wait_recv())

                @pl.when(pos > 0)
                def _():
                    pass_copy(way, c2, prv, big).start()

            pl.when((c2 >= 0) & (c2 < SMALL))(lambda: pass_step(False))
            pl.when((c2 >= SMALL) & (c2 < CHUNKS))(lambda: pass_step(True))

    def chain_steps(s0, n):
        def body(k, carry):
            chain_step(s0 + k)
            return carry
        lax.fori_loop(0, n, body, 0)

    def chain_end():
        for way in (0, 1):
            pos, nxt, prv = way_of(way)

            @pl.when(pos < DP - 1)
            def _():
                def body(c, carry):
                    chain_copy(way, c, nxt, True).wait_send()
                    return carry
                lax.fori_loop(CHUNKS - SLOTS, CHUNKS, body, 0)

            @pl.when(pos > 0)
            def _():
                def body(c, carry, big):
                    pass_copy(way, c, prv, big).wait_send()
                    return carry
                lax.fori_loop(0, SMALL, functools.partial(body, big=False), 0)
                lax.fori_loop(SMALL, CHUNKS, functools.partial(body, big=True), 0)

    def hat(ref, rs, k):
        return (ref[rs, :].astype(F32) - st_ref[rs, k:k + 1]) * st_ref[rs, k + 1:k + 2]

    def norm_back(d_norm, x_hat, rstd, gain):
        scaled = d_norm * gain
        scaled_mean = jnp.mean(scaled, axis=-1, keepdims=True)
        proj_mean = jnp.mean(scaled * x_hat, axis=-1, keepdims=True)
        return rstd * (scaled - scaled_mean - x_hat * proj_mean)

    def gain(k):
        return gn_ref[k:k + 1, :]

    def put_stats(k, ref):
        stat_t = jnp.transpose(ref[...])
        for b in range(TOK // 128):
            st_ref[b * 128:(b + 1) * 128, k:k + 1] = stat_t[:, b:b + 1]

    def put_gain(k, ref):
        wide = ref[...].astype(F32)
        for b in range(8):
            gn_ref[k:k + 1, b * 128:(b + 1) * 128] = wide[b:b + 1, :]

    def mate_copy(rnd, b):
        return pltpu.make_async_remote_copy(
            src_ref=part.at[at(par0, b)], dst_ref=recv_a.at[b], send_sem=pa_send.at[rnd, b],
            recv_sem=pa_recv.at[rnd, b], device_id=mate, device_id_type=MESH)

    def peer_copy(rnd, b):
        dst = (recv_b, recv_c)[rnd]
        return pltpu.make_async_remote_copy(
            src_ref=part.at[at(own0, b)], dst_ref=dst.at[b], send_sem=pb_send.at[rnd, b],
            recv_sem=pb_recv.at[rnd, b], device_id=peer, device_id_type=MESH)

    def chip_sum(rnd, b):
        mate_copy(rnd, b).wait_recv()
        ro = at(own0, b)
        part[ro, :] = (part[ro, :].astype(F32) + recv_a[b].astype(F32)).astype(BF16)
        peer_copy(rnd, b).start()

    def part_block(rnd, b, fn):
        rp = at(par0, b)
        part[rp, :] = fn(rp).astype(BF16)
        mate_copy(rnd, b).start()
        ro = at(own0, b)
        part[ro, :] = fn(ro).astype(BF16)

    def mlp(w1_ref, w2_ref, act_s, da_s):
        def w1_copy(j):
            return pltpu.make_async_copy(w1_hbm.at[:, rows(j)], w1_ref.at[:, rows(j)], in_sem.at[7 + j])

        def w2_copy(j):
            return pltpu.make_async_copy(w2_hbm.at[rows(j)], w2_ref.at[rows(j)], in_sem.at[11 + j])

        for i in range(NBLK):
            h_copy(i).start()
            if i == 0:
                w1_copy(0).start()
                w2_copy(0).start()
            dy_copy(i).start()
        for j in range(1, 4):
            w1_copy(j).start()
            w2_copy(j).start()
        put_stats(2, m2_ref)
        put_stats(3, r2_ref)
        put_gain(1, g2_ref)

        def act_block(rs, n2, cols):
            pre = dot_nn(n2, w1_ref[:, cols]).astype(BF16).astype(F32)
            th = jnp.tanh(GELU_C * (pre + 0.044715 * pre * pre * pre))
            act_s[rs, :] = (0.5 * pre * (1.0 + th)).astype(BF16)
            slope = 0.5 * (1.0 + th) + 0.5 * pre * (1.0 - th * th) * GELU_C * (1.0 + 0.134145 * pre * pre)
            da_s[rs, cols] = (dot_nt(dy_ref[rs, :], w2_ref[cols, :]) * slope).astype(BF16)

        def first(i, carry):
            h_copy(i).wait()
            n2 = (hat(h_ref, rows(i), 2) * gain(1)).astype(BF16)
            nrm[rows(i), :] = n2

            @pl.when(i == 0)
            def _():
                w1_copy(0).wait()
                w2_copy(0).wait()
            dy_copy(i).wait()
            act_block(rows(i), n2, slice(0, BLK))
            return carry
        lax.fori_loop(0, NBLK, first, 0)
        gb[0:BLK, :] = dot_tn(act_s[...], dy_ref[...])
        pl.semaphore_wait(barrier, peers)
        chain_step(0, True)

        def column(j, carry):
            w1_copy(j).wait()
            w2_copy(j).wait()

            def fwd(i, carry):
                rs = pl.ds(pl.multiple_of(i * 512, 512), 512)
                act_block(rs, nrm[rs, :], rows(j))
                pl.when(i < 2)(lambda: chain_step(3 * j - 2 + i, True))
                return carry
            lax.fori_loop(0, 3, fwd, 0)
            gb[rows(j), :] = dot_tn(act_s[...], dy_ref[...])
            chain_step(3 * j, True)
            return carry
        lax.fori_loop(1, DIM // BLK, column, 0)

        def dn2(b, carry):
            part_block(0, b, lambda rs: dot_nt(da_s[rs, :], w1_ref[...]))
            pl.when(b > 0)(lambda: chip_sum(0, b - 1))
            chain_step(10 + b, True)
            return carry
        lax.fori_loop(0, HBLK, dn2, 0)
        chip_sum(0, HBLK - 1)

        def up(j, carry):
            gb[at(DIM, j), :] = dot_tn(nrm[:, rows(j)], da_s[...])
            pl.when(lax.rem(j, 2) == 1)(lambda: chain_step(13 + lax.div(j, 2), True))
            return carry
        lax.fori_loop(0, DIM // BLK, up, 0)

    pl.run_scoped(mlp, pltpu.VMEM((DIM, DIM), BF16), pltpu.VMEM((DIM, DIM), BF16),
                  pltpu.VMEM((TOK, BLK), BF16), pltpu.VMEM((TOK, DIM), BF16))
    put_stats(0, m1_ref)
    put_stats(1, r1_ref)
    put_gain(0, g1_ref)

    def mid_copy(b):
        return pltpu.make_async_remote_copy(
            src_ref=dh_b.at[at(own0, b)], dst_ref=dh_b.at[at(own0, b)], send_sem=pd_send.at[0, b],
            recv_sem=pd_recv.at[0, b], device_id=mate, device_id_type=MESH)

    def out_copy(b):
        return pltpu.make_async_remote_copy(
            src_ref=part.at[at(own0, b)], dst_ref=part.at[at(own0, b)], send_sem=pd_send.at[1, b],
            recv_sem=pd_recv.at[1, b], device_id=mate, device_id_type=MESH)

    def attention(x_ref, wq_ref, wo_ref, qkv, d_qkv, o_s, do_s, acc_k, acc_v):
        x_copy = pltpu.make_async_copy(x_hbm, x_ref, in_sem.at[15])
        wq_copy = pltpu.make_async_copy(wq_hbm, wq_ref, in_sem.at[16])
        wo_copy = pltpu.make_async_copy(wo_hbm, wo_ref, in_sem.at[17])
        x_copy.start()
        wq_copy.start()
        wo_copy.start()
        x_copy.wait()
        wq_copy.wait()
        wo_copy.wait()

        def proj(i, carry):
            rs = rows(i)
            n1 = (hat(x_ref, rs, 0) * gain(0)).astype(BF16)
            nrm[rs, :] = n1
            qkv[rs, :] = dot_nt(n1, wq_ref[...]).astype(BF16)
            pl.when((i == 2) | (i == 4))(lambda: chain_step(14 + lax.div(i, 2), True))
            return carry
        lax.fori_loop(0, NBLK, proj, 0)

        def mid(b, carry):
            chain_step(17 + 2 * b)
            pl.when(b < 2)(lambda: chain_step(18 + 2 * b))
            peer_copy(0, b).wait_recv()
            ro = at(own0, b)
            d_norm = part[ro, :].astype(F32) + recv_b[b].astype(F32)
            dh = dy_ref[ro, :].astype(F32) + norm_back(d_norm, hat(h_ref, ro, 2), st_ref[ro, 3:4], gain(1))
            dh_f[rows(b), :] = dh
            dh_b[ro, :] = dh.astype(BF16)
            mid_copy(b).start()
            return carry
        lax.fori_loop(0, HBLK, mid, 0)
        for b in range(HBLK):
            mid_copy(b).wait_recv()

        def d_out(i, carry):
            do_s[rows(i), :] = dot_nt(dh_b[rows(i), :], wo_ref[...]).astype(BF16)
            return carry
        lax.fori_loop(0, NBLK, d_out, 0)

        lane = lax.broadcasted_iota(jnp.int32, (BLK, 128), 1)
        causal = lax.broadcasted_iota(jnp.int32, (BLK, BLK), 1) <= lax.broadcasted_iota(jnp.int32, (BLK, BLK), 0)
        zero = jnp.zeros((BLK, 128), BF16)

        def pair(p, carry):
            def cols(k):
                return pl.ds(pl.multiple_of(k * 256 + p * 128, 128), 128)
            polls = 0
            for i in reversed(range(NBLK)):
                span = (i + 1) * BLK
                rs = slice(i * BLK, span)
                k_all = qkv[0:span, cols(1)]
                v_all = qkv[0:span, cols(2)]
                outs, dqs = [], []
                dk = dv = None
                for hh in (0, 1):
                    mine = (lane < 64) if hh == 0 else (lane >= 64)
                    q = jnp.where(mine, qkv[rs, cols(0)], zero)
                    do = jnp.where(mine, do_s[rs, cols(0)], zero)
                    sc = dot_nt(q, k_all) * 0.125
                    last = jnp.where(causal, sc[:, span - BLK:], -1e30)
                    sc = jnp.concatenate([sc[:, :span - BLK], last], axis=1) if i else last
                    ex = jnp.exp(sc - jnp.max(sc, axis=-1, keepdims=True))
                    prob = ex * (1.0 / jnp.sum(ex, axis=-1, keepdims=True))
                    prob_lo = prob.astype(BF16)
                    outs.append(dot_nn(prob_lo, v_all))
                    dp = dot_nt(do, v_all)
                    ds = (prob * (dp - jnp.sum(prob * dp, axis=-1, keepdims=True)) * 0.125).astype(BF16)
                    dqs.append(dot_nn(ds, k_all))
                    dv_h = dot_tn(prob_lo, do)
                    dk_h = dot_tn(ds, q)
                    if i == NBLK - 1 and hh == 0:
                        acc_v[...] = dv_h
                        acc_k[...] = dk_h
                    else:
                        acc_v[0:span, :] += dv_h
                        acc_k[0:span, :] += dk_h
                    if (i >= 4 and hh == 0) or (i >= 2 and hh == 1) or (i == 0 and hh == 1):
                        chain_step(22 + p * 7 + polls)
                        polls += 1
                o_s[rs, cols(0)] = jnp.where(lane < 64, outs[0], outs[1]).astype(BF16)
                d_qkv[rs, cols(0)] = jnp.where(lane < 64, dqs[0], dqs[1]).astype(BF16)
            d_qkv[:, cols(1)] = acc_k[...].astype(BF16)
            d_qkv[:, cols(2)] = acc_v[...].astype(BF16)
            return carry
        lax.fori_loop(0, 2, pair, 0)

        gb[2 * DIM:2 * DIM + BLK, :] = dot_tn(o_s[...], dh_b[...])
        chain_step(36)

        def w_qkv(j, carry):
            gb[at(2 * DIM + BLK, j), :] = dot_tn(d_qkv[:, rows(j)], nrm[...])
            chain_step(37 + j)
            return carry
        lax.fori_loop(0, 3, w_qkv, 0)

        for b in range(HBLK):
            mate_copy(0, b).wait_send()
            peer_copy(0, b).wait_send()
            mid_copy(b).wait_send()

        def dn1(b, carry):
            part_block(1, b, lambda rs: dot_nn(d_qkv[rs, :], wq_ref[...]))
            pl.when(b > 0)(lambda: chip_sum(1, b - 1))
            chain_step(40 + b)
            return carry
        lax.fori_loop(0, HBLK, dn1, 0)
        chip_sum(1, HBLK - 1)

        def final(b, carry):
            chain_step(43 + 3 * b)
            chain_step(44 + 3 * b)
            chain_step(45 + 3 * b)
            peer_copy(1, b).wait_recv()
            peer_copy(1, b).wait_send()
            ro = at(own0, b)
            d_norm = part[ro, :].astype(F32) + recv_c[b].astype(F32)
            dx = dh_f[rows(b), :] + norm_back(d_norm, hat(x_ref, ro, 0), st_ref[ro, 1:2], gain(0))
            part[ro, :] = dx.astype(BF16)
            out_copy(b).start()
            return carry
        for b in range(HBLK):
            mate_copy(1, b).wait_send()
        pl.semaphore_signal(mate_done, inc=1, device_id=mate, device_id_type=MESH)
        pl.semaphore_wait(mate_done, 1)
        lax.fori_loop(0, HBLK, final, 0)

    pl.run_scoped(attention, pltpu.VMEM((TOK, DIM), BF16), pltpu.VMEM((768, DIM), BF16), pltpu.VMEM((BLK, DIM), BF16),
                  pltpu.VMEM((TOK, 768), BF16), pltpu.VMEM((TOK, 768), BF16),
                  pltpu.VMEM((TOK, BLK), BF16), pltpu.VMEM((TOK, BLK), BF16),
                  pltpu.VMEM((TOK, 128), F32), pltpu.VMEM((TOK, 128), F32))

    chain_steps(43 + 3 * HBLK, STEPS - 43 - 3 * HBLK)
    chain_end()
    for b in range(HBLK):
        out_copy(b).wait()


def close_kernel(dx_ref, fb_ref, x_out, q_out, o_out, up_out, down_out, sem):
    copies = [pltpu.make_async_copy(fb_ref.at[0:DIM], down_out, sem.at[0]),
              pltpu.make_async_copy(fb_ref.at[DIM:2 * DIM], up_out, sem.at[1]),
              pltpu.make_async_copy(dx_ref, x_out, sem.at[2]),
              pltpu.make_async_copy(fb_ref.at[2 * DIM:2 * DIM + BLK], o_out, sem.at[3]),
              pltpu.make_async_copy(fb_ref.at[2 * DIM + BLK:ROWS], q_out, sem.at[4])]
    for copy in copies:
        copy.start()
    for copy in copies:
        copy.wait()


def solution(mesh):
    row_spec = P(('pod', 'dp'), None)
    stat_spec = P(('pod', 'dp'))
    in_specs = (row_spec, row_spec, stat_spec, stat_spec, stat_spec, stat_spec, P(None), P(None), row_spec,
                P(None, None, 'tp', None), P('tp', None, None), P(None, 'tp'), P('tp', None))
    out_specs = (row_spec, P('pod', None, 'tp', None), P(('pod', 'tp'), None, None), P('pod', 'tp'), P(('pod', 'tp'), None))

    vmem = pl.BlockSpec(memory_space=pltpu.VMEM)
    hbm = pl.BlockSpec(memory_space=pl.ANY)
    dma = pltpu.SemaphoreType.DMA
    scratch = [
        pltpu.VMEM((ROWS, DIM), F32),
        pltpu.VMEM((2, SLOTS, CROWS, DIM), F32),
        pltpu.VMEM((TOK, DIM), BF16),
        pltpu.VMEM((HBLK, BLK, DIM), BF16),
        pltpu.VMEM((HBLK, BLK, DIM), BF16),
        pltpu.VMEM((HBLK, BLK, DIM), BF16),
        pltpu.VMEM((HALF, DIM), F32),
        pltpu.VMEM((TOK, DIM), BF16),
        pltpu.VMEM((TOK, DIM), BF16),
        pltpu.VMEM((TOK, DIM), BF16),
        pltpu.VMEM((TOK, 4), F32),
        pltpu.VMEM((2, DIM), F32),
        dma((2, SLOTS)), dma((2, SLOTS)), pltpu.SemaphoreType.REGULAR((2,)),
        dma((2, CHUNKS)), dma((2, CHUNKS)),
        dma((2, HBLK)), dma((2, HBLK)), dma((2, HBLK)), dma((2, HBLK)),
        dma((2, HBLK)), dma((2, HBLK)), dma((24,)), pltpu.SemaphoreType.REGULAR,
    ]
    layer = pl.pallas_call(
        layer_kernel,
        out_shape=(OUT_SPACE((TOK, DIM), BF16), OUT_SPACE((ROWS, DIM), BF16)),
        in_specs=[hbm] * 3 + [vmem] * 6 + [hbm] * 4,
        out_specs=(vmem, vmem),
        scratch_shapes=scratch,
        compiler_params=pltpu.CompilerParams(collective_id=0, has_side_effects=True, vmem_limit_bytes=VMEM_LIMIT),
        name='layer_backward')

    close = pl.pallas_call(
        close_kernel,
        out_shape=tuple(jax.ShapeDtypeStruct((r, DIM), BF16) for r in (TOK, 768, BLK, DIM, DIM)),
        in_specs=[vmem, vmem],
        out_specs=(hbm,) * 5,
        scratch_shapes=[dma((5,))],
        compiler_params=pltpu.CompilerParams(vmem_limit_bytes=CLOSE_LIMIT),
        name='close')

    def local_step(x_saved, h_saved, mean_one, rstd_one, mean_two, rstd_two, gain_one, gain_two, grad_y, w_qkv, w_proj, w_up, w_down):
        small = [a.reshape(-1, 128) for a in (mean_one, rstd_one, mean_two, rstd_two, gain_one, gain_two)]
        wq_t = jnp.transpose(w_qkv, (1, 2, 3, 0)).reshape(768, DIM)
        grad_x, grads = layer(x_saved, h_saved, grad_y, *small, wq_t, w_proj.reshape(BLK, DIM), w_up, w_down)
        grad_x, grad_qkv, grad_proj, grad_up, grad_down = close(grad_x, grads)
        grad_qkv = jnp.transpose(grad_qkv.reshape(3, 4, 64, DIM), (3, 0, 1, 2))
        return grad_x, grad_qkv, grad_proj.reshape(4, 64, DIM), grad_up, grad_down

    return jax.shard_map(local_step, mesh=mesh, in_specs=in_specs, out_specs=out_specs, check_vma=False)
```

```python
import functools
import math
import jax
import jax.numpy as jnp
from jax import lax
from jax.experimental import pallas as pl
from jax.experimental.pallas import tpu as pltpu
from jax.sharding import PartitionSpec as P

GELU_C = math.sqrt(2.0 / math.pi)
MESH = pl.DeviceIdType.MESH
F32 = jnp.float32
BF16 = jnp.bfloat16

TOK = 1536
DIM = 1024
BLK = 256
HALF = TOK // 2
NBLK = TOK // BLK
HBLK = HALF // BLK
CROWS = 32
SROWS = 16
SMALL = 8
ROWS = 3072
CHUNKS = SMALL + (ROWS - 2 * SROWS * SMALL) // (2 * CROWS)
SLOTS = 8
LAG = 2
LAG_BACK = 2
HOLD = 0
DP = 4
OUT_SPACE = pltpu.VMEM
VMEM_LIMIT = 54 * 2 ** 20
CLOSE_LIMIT = 1 * 2 ** 20
STEPS = CHUNKS + (LAG + LAG_BACK) * (DP - 1) + HOLD


def dot_nn(a, b):
    return lax.dot_general(a, b, (((1,), (0,)), ((), ())), preferred_element_type=F32)


def dot_nt(a, b):
    return lax.dot_general(a, b, (((1,), (1,)), ((), ())), preferred_element_type=F32)


def dot_tn(a, b):
    return lax.dot_general(a, b, (((0,), (0,)), ((), ())), preferred_element_type=F32)


def layer_kernel(x_hbm, h_hbm, dy_hbm, m1_ref, r1_ref, m2_ref, r2_ref, g1_ref, g2_ref, wq_hbm, wo_hbm, w1_hbm, w2_hbm,
                 part, fb_ref,
                 gb, land, nrm, recv_a, recv_b, recv_c, dh_f, dh_b, h_ref, dy_ref, st_ref, gn_ref,
                 ch_send, ch_recv, ch_free, fb_send, fb_recv,
                 pa_send, pa_recv, pb_send, pb_recv, pd_send, pd_recv, in_sem, mate_done):
    pod, z, tp = lax.axis_index('pod'), lax.axis_index('dp'), lax.axis_index('tp')
    core = lax.rem(tp, 2)
    mate = (pod, z, tp + 1 - 2 * core)
    peer = (pod, z, lax.rem(tp + 2, 4))
    z_hi = jnp.minimum(z + 1, DP - 1)
    z_lo = jnp.maximum(z - 1, 0)
    own0 = core * HALF
    par0 = HALF - own0

    def rows(i):
        return pl.ds(pl.multiple_of(i * BLK, BLK), BLK)

    def at(base, b):
        return pl.ds(pl.multiple_of(base + b * BLK, BLK), BLK)

    def h_copy(i):
        return pltpu.make_async_copy(h_hbm.at[rows(i)], h_ref.at[rows(i)], in_sem.at[i])

    def dy_copy(i):
        return pltpu.make_async_copy(dy_hbm.at[rows(i)], dy_ref.at[rows(i)], in_sem.at[18 + i])

    barrier = pltpu.get_barrier_semaphore()
    for dev in (mate, peer):
        pl.semaphore_signal(barrier, inc=1, device_id=dev, device_id_type=MESH)
    pl.when(z < DP - 1)(lambda: pl.semaphore_signal(barrier, inc=1, device_id=(pod, z_hi, tp), device_id_type=MESH))
    pl.when(z > 0)(lambda: pl.semaphore_signal(barrier, inc=1, device_id=(pod, z_lo, tp), device_id_type=MESH))
    peers = 2 + jnp.where(z < DP - 1, 1, 0) + jnp.where(z > 0, 1, 0)

    def way_of(way):
        if way == 0:
            return z, (pod, z_hi, tp), (pod, z_lo, tp)
        return DP - 1 - z, (pod, z_lo, tp), (pod, z_hi, tp)

    def rows_of(way, c, big):
        if big:
            start = 2 * SROWS * SMALL + (c - SMALL) * (2 * CROWS) + way * CROWS
            return pl.ds(pl.multiple_of(start, CROWS), CROWS)
        return pl.ds(pl.multiple_of(c * (2 * SROWS) + way * SROWS, SROWS), SROWS)

    def land_at(way, c, big):
        return land.at[way, lax.rem(c, SLOTS), pl.ds(0, CROWS if big else SROWS)]

    def chain_copy(way, c, nxt, big):
        slot = lax.rem(c, SLOTS)
        return pltpu.make_async_remote_copy(
            src_ref=gb.at[rows_of(way, c, big)], dst_ref=land_at(way, c, big), send_sem=ch_send.at[way, slot],
            recv_sem=ch_recv.at[way, slot], device_id=nxt, device_id_type=MESH)

    def pass_copy(way, c, prv, big):
        return pltpu.make_async_remote_copy(
            src_ref=fb_ref.at[rows_of(way, c, big)], dst_ref=fb_ref.at[rows_of(way, c, big)], send_sem=fb_send.at[way, c],
            recv_sem=fb_recv.at[way, c], device_id=prv, device_id_type=MESH)

    def chain_step(s, early=False):
        for way in (0, 1):
            pos, nxt, prv = way_of(way)
            c = s - LAG * pos

            def reduce_step(big):
                rs = rows_of(way, c, big)

                @pl.when(pos > 0)
                def _():
                    chain_copy(way, c, nxt, big).wait_recv()
                    total = gb[rs, :] + land_at(way, c, big)[...]

                    @pl.when(pos < DP - 1)
                    def _():
                        gb[rs, :] = total

                    @pl.when(pos == DP - 1)
                    def _():
                        fb_ref[rs, :] = total.astype(BF16)

                    @pl.when(c < CHUNKS - SLOTS)
                    def _():
                        pl.semaphore_signal(ch_free.at[way], inc=1, device_id=prv, device_id_type=MESH)

                @pl.when(pos < DP - 1)
                def _():
                    @pl.when(c >= SLOTS)
                    def _():
                        pl.semaphore_wait(ch_free.at[way], 1)
                    pl.when((c >= SLOTS) & (c < SLOTS + SMALL))(lambda: chain_copy(way, c - SLOTS, nxt, False).wait_send())
                    pl.when(c >= SLOTS + SMALL)(lambda: chain_copy(way, c - SLOTS, nxt, True).wait_send())
                    chain_copy(way, c, nxt, big).start()

            if early:
                pl.when((c >= 0) & (c < SMALL))(lambda: reduce_step(False))
            pl.when((c >= SMALL) & (c < CHUNKS))(lambda: reduce_step(True))

            c2 = s - HOLD - LAG * (DP - 1) - LAG_BACK * (DP - 1 - pos)

            def pass_step(big):
                pl.when(pos < DP - 1)(lambda: pass_copy(way, c2, prv, big).wait_recv())

                @pl.when(pos > 0)
                def _():
                    pass_copy(way, c2, prv, big).start()

            pl.when((c2 >= 0) & (c2 < SMALL))(lambda: pass_step(False))
            pl.when((c2 >= SMALL) & (c2 < CHUNKS))(lambda: pass_step(True))

    def chain_steps(s0, n):
        def body(k, carry):
            chain_step(s0 + k)
            return carry
        lax.fori_loop(0, n, body, 0)

    def chain_end():
        for way in (0, 1):
            pos, nxt, prv = way_of(way)

            @pl.when(pos < DP - 1)
            def _():
                def body(c, carry):
                    chain_copy(way, c, nxt, True).wait_send()
                    return carry
                lax.fori_loop(CHUNKS - SLOTS, CHUNKS, body, 0)

            @pl.when(pos > 0)
            def _():
                def body(c, carry, big):
                    pass_copy(way, c, prv, big).wait_send()
                    return carry
                lax.fori_loop(0, SMALL, functools.partial(body, big=False), 0)
                lax.fori_loop(SMALL, CHUNKS, functools.partial(body, big=True), 0)

    def hat(ref, rs, k):
        return (ref[rs, :].astype(F32) - st_ref[rs, k:k + 1]) * st_ref[rs, k + 1:k + 2]

    def norm_back(d_norm, x_hat, rstd, gain):
        scaled = d_norm * gain
        scaled_mean = jnp.mean(scaled, axis=-1, keepdims=True)
        proj_mean = jnp.mean(scaled * x_hat, axis=-1, keepdims=True)
        return rstd * (scaled - scaled_mean - x_hat * proj_mean)

    def gain(k):
        return gn_ref[k:k + 1, :]

    def put_stats(k, ref):
        stat_t = jnp.transpose(ref[...])
        for b in range(TOK // 128):
            st_ref[b * 128:(b + 1) * 128, k:k + 1] = stat_t[:, b:b + 1]

    def put_gain(k, ref):
        wide = ref[...].astype(F32)
        for b in range(8):
            gn_ref[k:k + 1, b * 128:(b + 1) * 128] = wide[b:b + 1, :]

    def mate_copy(rnd, b):
        return pltpu.make_async_remote_copy(
            src_ref=part.at[at(par0, b)], dst_ref=recv_a.at[b], send_sem=pa_send.at[rnd, b],
            recv_sem=pa_recv.at[rnd, b], device_id=mate, device_id_type=MESH)

    def peer_copy(rnd, b):
        dst = (recv_b, recv_c)[rnd]
        return pltpu.make_async_remote_copy(
            src_ref=part.at[at(own0, b)], dst_ref=dst.at[b], send_sem=pb_send.at[rnd, b],
            recv_sem=pb_recv.at[rnd, b], device_id=peer, device_id_type=MESH)

    def chip_sum(rnd, b):
        mate_copy(rnd, b).wait_recv()
        ro = at(own0, b)
        part[ro, :] = (part[ro, :].astype(F32) + recv_a[b].astype(F32)).astype(BF16)
        peer_copy(rnd, b).start()

    def part_block(rnd, b, fn):
        rp = at(par0, b)
        part[rp, :] = fn(rp).astype(BF16)
        mate_copy(rnd, b).start()
        ro = at(own0, b)
        part[ro, :] = fn(ro).astype(BF16)

    def mlp(w1_ref, w2_ref, act_s, da_s):
        def w1_copy(j):
            return pltpu.make_async_copy(w1_hbm.at[:, rows(j)], w1_ref.at[:, rows(j)], in_sem.at[7 + j])

        def w2_copy(j):
            return pltpu.make_async_copy(w2_hbm.at[rows(j)], w2_ref.at[rows(j)], in_sem.at[11 + j])

        for i in range(NBLK):
            h_copy(i).start()
            if i == 0:
                w1_copy(0).start()
                w2_copy(0).start()
            dy_copy(i).start()
        for j in range(1, 4):
            w1_copy(j).start()
            w2_copy(j).start()
        put_stats(2, m2_ref)
        put_stats(3, r2_ref)
        put_gain(1, g2_ref)

        def act_block(rs, n2, cols):
            pre = dot_nn(n2, w1_ref[:, cols]).astype(BF16).astype(F32)
            th = jnp.tanh(GELU_C * (pre + 0.044715 * pre * pre * pre))
            act_s[rs, :] = (0.5 * pre * (1.0 + th)).astype(BF16)
            slope = 0.5 * (1.0 + th) + 0.5 * pre * (1.0 - th * th) * GELU_C * (1.0 + 0.134145 * pre * pre)
            da_s[rs, cols] = (dot_nt(dy_ref[rs, :], w2_ref[cols, :]) * slope).astype(BF16)

        def first(i, carry):
            h_copy(i).wait()
            n2 = (hat(h_ref, rows(i), 2) * gain(1)).astype(BF16)
            nrm[rows(i), :] = n2

            @pl.when(i == 0)
            def _():
                w1_copy(0).wait()
                w2_copy(0).wait()
            dy_copy(i).wait()
            act_block(rows(i), n2, slice(0, BLK))
            return carry
        lax.fori_loop(0, NBLK, first, 0)
        gb[0:BLK, :] = dot_tn(act_s[...], dy_ref[...])
        pl.semaphore_wait(barrier, peers)
        chain_step(0, True)

        def column(j, carry):
            w1_copy(j).wait()
            w2_copy(j).wait()

            def fwd(i, carry):
                rs = pl.ds(pl.multiple_of(i * 512, 512), 512)
                act_block(rs, nrm[rs, :], rows(j))
                pl.when(i < 2)(lambda: chain_step(3 * j - 2 + i, True))
                return carry
            lax.fori_loop(0, 3, fwd, 0)
            gb[rows(j), :] = dot_tn(act_s[...], dy_ref[...])
            chain_step(3 * j, True)
            return carry
        lax.fori_loop(1, DIM // BLK, column, 0)

        def dn2(b, carry):
            part_block(0, b, lambda rs: dot_nt(da_s[rs, :], w1_ref[...]))
            pl.when(b > 0)(lambda: chip_sum(0, b - 1))
            chain_step(10 + b, True)
            return carry
        lax.fori_loop(0, HBLK, dn2, 0)
        chip_sum(0, HBLK - 1)

        def up(j, carry):
            gb[at(DIM, j), :] = dot_tn(nrm[:, rows(j)], da_s[...])
            pl.when(lax.rem(j, 2) == 1)(lambda: chain_step(13 + lax.div(j, 2), True))
            return carry
        lax.fori_loop(0, DIM // BLK, up, 0)

    pl.run_scoped(mlp, pltpu.VMEM((DIM, DIM), BF16), pltpu.VMEM((DIM, DIM), BF16),
                  pltpu.VMEM((TOK, BLK), BF16), pltpu.VMEM((TOK, DIM), BF16))
    put_stats(0, m1_ref)
    put_stats(1, r1_ref)
    put_gain(0, g1_ref)

    def mid_copy(b):
        return pltpu.make_async_remote_copy(
            src_ref=dh_b.at[at(own0, b)], dst_ref=dh_b.at[at(own0, b)], send_sem=pd_send.at[0, b],
            recv_sem=pd_recv.at[0, b], device_id=mate, device_id_type=MESH)

    def out_copy(b):
        return pltpu.make_async_remote_copy(
            src_ref=part.at[at(own0, b)], dst_ref=part.at[at(own0, b)], send_sem=pd_send.at[1, b],
            recv_sem=pd_recv.at[1, b], device_id=mate, device_id_type=MESH)

    def attention(x_ref, wq_ref, wo_ref, qkv, d_qkv, o_s, do_s, acc_k, acc_v):
        x_copy = pltpu.make_async_copy(x_hbm, x_ref, in_sem.at[15])
        wq_copy = pltpu.make_async_copy(wq_hbm, wq_ref, in_sem.at[16])
        wo_copy = pltpu.make_async_copy(wo_hbm, wo_ref, in_sem.at[17])
        x_copy.start()
        wq_copy.start()
        wo_copy.start()
        x_copy.wait()
        wq_copy.wait()
        wo_copy.wait()

        def proj(i, carry):
            rs = rows(i)
            n1 = (hat(x_ref, rs, 0) * gain(0)).astype(BF16)
            nrm[rs, :] = n1
            qkv[rs, :] = dot_nt(n1, wq_ref[...]).astype(BF16)
            pl.when((i == 2) | (i == 4))(lambda: chain_step(14 + lax.div(i, 2), True))
            return carry
        lax.fori_loop(0, NBLK, proj, 0)

        def mid(b, carry):
            chain_step(17 + 2 * b)
            pl.when(b < 2)(lambda: chain_step(18 + 2 * b))
            peer_copy(0, b).wait_recv()
            ro = at(own0, b)
            d_norm = part[ro, :].astype(F32) + recv_b[b].astype(F32)
            dh = dy_ref[ro, :].astype(F32) + norm_back(d_norm, hat(h_ref, ro, 2), st_ref[ro, 3:4], gain(1))
            dh_f[rows(b), :] = dh
            dh_b[ro, :] = dh.astype(BF16)
            mid_copy(b).start()
            return carry
        lax.fori_loop(0, HBLK, mid, 0)
        for b in range(HBLK):
            mid_copy(b).wait_recv()

        def d_out(i, carry):
            do_s[rows(i), :] = dot_nt(dh_b[rows(i), :], wo_ref[...]).astype(BF16)
            return carry
        lax.fori_loop(0, NBLK, d_out, 0)

        lane = lax.broadcasted_iota(jnp.int32, (BLK, 128), 1)
        causal = lax.broadcasted_iota(jnp.int32, (BLK, BLK), 1) <= lax.broadcasted_iota(jnp.int32, (BLK, BLK), 0)
        zero = jnp.zeros((BLK, 128), BF16)

        def pair(p, carry):
            def cols(k):
                return pl.ds(pl.multiple_of(k * 256 + p * 128, 128), 128)
            polls = 0
            for i in reversed(range(NBLK)):
                span = (i + 1) * BLK
                rs = slice(i * BLK, span)
                k_all = qkv[0:span, cols(1)]
                v_all = qkv[0:span, cols(2)]
                outs, dqs = [], []
                dk = dv = None
                for hh in (0, 1):
                    mine = (lane < 64) if hh == 0 else (lane >= 64)
                    q = jnp.where(mine, qkv[rs, cols(0)], zero)
                    do = jnp.where(mine, do_s[rs, cols(0)], zero)
                    sc = dot_nt(q, k_all) * 0.125
                    last = jnp.where(causal, sc[:, span - BLK:], -1e30)
                    sc = jnp.concatenate([sc[:, :span - BLK], last], axis=1) if i else last
                    ex = jnp.exp(sc - jnp.max(sc, axis=-1, keepdims=True))
                    prob = ex * (1.0 / jnp.sum(ex, axis=-1, keepdims=True))
                    prob_lo = prob.astype(BF16)
                    outs.append(dot_nn(prob_lo, v_all))
                    dp = dot_nt(do, v_all)
                    ds = (prob * (dp - jnp.sum(prob * dp, axis=-1, keepdims=True)) * 0.125).astype(BF16)
                    dqs.append(dot_nn(ds, k_all))
                    dv_h = dot_tn(prob_lo, do)
                    dk_h = dot_tn(ds, q)
                    if i == NBLK - 1 and hh == 0:
                        acc_v[...] = dv_h
                        acc_k[...] = dk_h
                    else:
                        acc_v[0:span, :] += dv_h
                        acc_k[0:span, :] += dk_h
                    if (i >= 4 and hh == 0) or (i >= 2 and hh == 1) or (i == 0 and hh == 1):
                        chain_step(22 + p * 7 + polls)
                        polls += 1
                o_s[rs, cols(0)] = jnp.where(lane < 64, outs[0], outs[1]).astype(BF16)
                d_qkv[rs, cols(0)] = jnp.where(lane < 64, dqs[0], dqs[1]).astype(BF16)
            d_qkv[:, cols(1)] = acc_k[...].astype(BF16)
            d_qkv[:, cols(2)] = acc_v[...].astype(BF16)
            return carry
        lax.fori_loop(0, 2, pair, 0)

        gb[2 * DIM:2 * DIM + BLK, :] = dot_tn(o_s[...], dh_b[...])
        chain_step(36)

        def w_qkv(j, carry):
            gb[at(2 * DIM + BLK, j), :] = dot_tn(d_qkv[:, rows(j)], nrm[...])
            chain_step(37 + j)
            return carry
        lax.fori_loop(0, 3, w_qkv, 0)

        for b in range(HBLK):
            mate_copy(0, b).wait_send()
            peer_copy(0, b).wait_send()
            mid_copy(b).wait_send()

        def dn1(b, carry):
            part_block(1, b, lambda rs: dot_nn(d_qkv[rs, :], wq_ref[...]))
            pl.when(b > 0)(lambda: chip_sum(1, b - 1))
            chain_step(40 + b)
            return carry
        lax.fori_loop(0, HBLK, dn1, 0)
        chip_sum(1, HBLK - 1)

        def final(b, carry):
            chain_step(43 + 3 * b)
            chain_step(44 + 3 * b)
            chain_step(45 + 3 * b)
            peer_copy(1, b).wait_recv()
            peer_copy(1, b).wait_send()
            ro = at(own0, b)
            d_norm = part[ro, :].astype(F32) + recv_c[b].astype(F32)
            dx = dh_f[rows(b), :] + norm_back(d_norm, hat(x_ref, ro, 0), st_ref[ro, 1:2], gain(0))
            part[ro, :] = dx.astype(BF16)
            out_copy(b).start()
            return carry
        for b in range(HBLK):
            mate_copy(1, b).wait_send()
        pl.semaphore_signal(mate_done, inc=1, device_id=mate, device_id_type=MESH)
        pl.semaphore_wait(mate_done, 1)
        lax.fori_loop(0, HBLK, final, 0)

    pl.run_scoped(attention, pltpu.VMEM((TOK, DIM), BF16), pltpu.VMEM((768, DIM), BF16), pltpu.VMEM((BLK, DIM), BF16),
                  pltpu.VMEM((TOK, 768), BF16), pltpu.VMEM((TOK, 768), BF16),
                  pltpu.VMEM((TOK, BLK), BF16), pltpu.VMEM((TOK, BLK), BF16),
                  pltpu.VMEM((TOK, 128), F32), pltpu.VMEM((TOK, 128), F32))

    chain_steps(43 + 3 * HBLK, STEPS - 43 - 3 * HBLK)
    chain_end()
    for b in range(HBLK):
        out_copy(b).wait()


def close_kernel(dx_ref, fb_ref, x_out, q_out, o_out, up_out, down_out, sem):
    copies = [pltpu.make_async_copy(fb_ref.at[0:DIM], down_out, sem.at[0]),
              pltpu.make_async_copy(fb_ref.at[DIM:2 * DIM], up_out, sem.at[1]),
              pltpu.make_async_copy(dx_ref, x_out, sem.at[2]),
              pltpu.make_async_copy(fb_ref.at[2 * DIM:2 * DIM + BLK], o_out, sem.at[3]),
              pltpu.make_async_copy(fb_ref.at[2 * DIM + BLK:ROWS], q_out, sem.at[4])]
    for copy in copies:
        copy.start()
    for copy in copies:
        copy.wait()


def solution(mesh):
    row_spec = P(('pod', 'dp'), None)
    stat_spec = P(('pod', 'dp'))
    in_specs = (row_spec, row_spec, stat_spec, stat_spec, stat_spec, stat_spec, P(None), P(None), row_spec,
                P(None, None, 'tp', None), P('tp', None, None), P(None, 'tp'), P('tp', None))
    out_specs = (row_spec, P('pod', None, 'tp', None), P(('pod', 'tp'), None, None), P('pod', 'tp'), P(('pod', 'tp'), None))

    vmem = pl.BlockSpec(memory_space=pltpu.VMEM)
    hbm = pl.BlockSpec(memory_space=pl.ANY)
    dma = pltpu.SemaphoreType.DMA
    scratch = [
        pltpu.VMEM((ROWS, DIM), F32),
        pltpu.VMEM((2, SLOTS, CROWS, DIM), F32),
        pltpu.VMEM((TOK, DIM), BF16),
        pltpu.VMEM((HBLK, BLK, DIM), BF16),
        pltpu.VMEM((HBLK, BLK, DIM), BF16),
        pltpu.VMEM((HBLK, BLK, DIM), BF16),
        pltpu.VMEM((HALF, DIM), F32),
        pltpu.VMEM((TOK, DIM), BF16),
        pltpu.VMEM((TOK, DIM), BF16),
        pltpu.VMEM((TOK, DIM), BF16),
        pltpu.VMEM((TOK, 4), F32),
        pltpu.VMEM((2, DIM), F32),
        dma((2, SLOTS)), dma((2, SLOTS)), pltpu.SemaphoreType.REGULAR((2,)),
        dma((2, CHUNKS)), dma((2, CHUNKS)),
        dma((2, HBLK)), dma((2, HBLK)), dma((2, HBLK)), dma((2, HBLK)),
        dma((2, HBLK)), dma((2, HBLK)), dma((24,)), pltpu.SemaphoreType.REGULAR,
    ]
    layer = pl.pallas_call(
        layer_kernel,
        out_shape=(OUT_SPACE((TOK, DIM), BF16), OUT_SPACE((ROWS, DIM), BF16)),
        in_specs=[hbm] * 3 + [vmem] * 6 + [hbm] * 4,
        out_specs=(vmem, vmem),
        scratch_shapes=scratch,
        compiler_params=pltpu.CompilerParams(collective_id=0, has_side_effects=True, vmem_limit_bytes=VMEM_LIMIT),
        name='layer_backward')

    close = pl.pallas_call(
        close_kernel,
        out_shape=tuple(jax.ShapeDtypeStruct((r, DIM), BF16) for r in (TOK, 768, BLK, DIM, DIM)),
        in_specs=[vmem, vmem],
        out_specs=(hbm,) * 5,
        scratch_shapes=[dma((5,))],
        compiler_params=pltpu.CompilerParams(vmem_limit_bytes=CLOSE_LIMIT),
        name='close')

    def local_step(x_saved, h_saved, mean_one, rstd_one, mean_two, rstd_two, gain_one, gain_two, grad_y, w_qkv, w_proj, w_up, w_down):
        small = [a.reshape(-1, 128) for a in (mean_one, rstd_one, mean_two, rstd_two, gain_one, gain_two)]
        wq_t = jnp.transpose(w_qkv, (1, 2, 3, 0)).reshape(768, DIM)
        grad_x, grads = layer(x_saved, h_saved, grad_y, *small, wq_t, w_proj.reshape(BLK, DIM), w_up, w_down)
        grad_x, grad_qkv, grad_proj, grad_up, grad_down = close(grad_x, grads)
        grad_qkv = jnp.transpose(grad_qkv.reshape(3, 4, 64, DIM), (3, 0, 1, 2))
        return grad_x, grad_qkv, grad_proj.reshape(4, 64, DIM), grad_up, grad_down

    return jax.shard_map(local_step, mesh=mesh, in_specs=in_specs, out_specs=out_specs, check_vma=False)
```
